256 devices in a mesh: section: 16 (over z_lo, x), dp: 16 (over z_hi, y, core).
Axes of the slice: x: 4, y: 4, z: 8 (z_hi: 2, z_lo: 4; z = z_hi * 4 + z_lo), core: 2. Of those that a mesh axis runs over, the one named last changes fastest.
Arguments:
- carry_act: bfloat16 [16, 128, 2304], P('section', 'dp'), may hold values from -6 to 6
- carry_act_tan: bfloat16 [16, 128, 2304], P('section', 'dp'), may hold values from -6 to 6
- carry_adj: bfloat16 [16, 128, 2304], P('section', 'dp'), may hold values from -0.75 to 0.75
- carry_adj_tan: bfloat16 [16, 128, 2304], P('section', 'dp'), may hold values from -0.75 to 0.75
- fresh_act: bfloat16 [2, 128, 2304], P(None, 'dp'), may hold values from -6 to 6
- loss_cot: bfloat16 [2, 128, 2304], P(None, 'dp'), may hold values from -0.75 to 0.75
- stash_act: bfloat16 [16, 2, 128, 2304], P('section', None, 'dp'), may hold values from -6 to 6
- stash_act_tan: bfloat16 [16, 2, 128, 2304], P('section', None, 'dp'), may hold values from -6 to 6
- norm_gain: bfloat16 [16, 2304], P('section'), may hold values from 0.25 to 1.75
- up_weight: bfloat16 [16, 2304, 4608], P('section', None, 'dp'), may hold values from -0.125 to 0.125
- down_weight: bfloat16 [16, 4608, 2304], P('section', 'dp'), may hold values from -0.09375 to 0.09375
- up_dir: bfloat16 [16, 2304, 4608], P('section', None, 'dp'), may hold values from -0.125 to 0.125
- down_dir: bfloat16 [16, 4608, 2304], P('section', 'dp'), may hold values from -0.09375 to 0.09375
Outputs:
- next_act: bfloat16 [16, 128, 2304], P('section', 'dp')
- next_act_tan: bfloat16 [16, 128, 2304], P('section', 'dp')
- next_adj: bfloat16 [16, 128, 2304], P('section', 'dp')
- next_adj_tan: bfloat16 [16, 128, 2304], P('section', 'dp')
- hvp_up: bfloat16 [16, 2304, 4608], P('section', None, 'dp')
- hvp_down: bfloat16 [16, 4608, 2304], P('section', 'dp')
The draws below stay inside these ranges and needn't reach their ends.
All inputs are finite; a program needn't handle non-finite values.
Results may differ from the reference program's by a relative error of at most 0.02.
Values may be sent and summed in bfloat16 or wider, within the bound.
A program may use at most 128 MiB of HBM per device.

```python
import jax
import jax.numpy as jnp
from jax import lax

D = 2304
FF = 4608
TICKS = 2
TOKENS = 128
SECTIONS = 16
N_DP = 16


def block_levels(key, dims, split, low, top_value):
    factor_of = 1.0
    for position, blocks in split:
        draws = jax.random.uniform(jax.random.fold_in(jax.random.fold_in(key, 6), position), (blocks,), jnp.float32, low / len(split), top_value / len(split))
        factor_of = factor_of * jnp.repeat(jnp.exp(draws), dims[position] // blocks).reshape((-1,) + (1,) * (len(dims) - 1 - position))
    return factor_of


def noise(own_key, dims, scale, reach, cuts=(), dtype=jnp.bfloat16):
    entries = scale * jax.random.normal(own_key, dims, jnp.float32)
    if cuts:
        entries = entries * block_levels(own_key, dims, cuts, -0.22, 0.18)
    return jnp.clip(entries, -reach, reach).astype(dtype)


def setup_inputs(seed: int = 0) -> dict:
    splits = jax.random.split(jax.random.key(seed), 14)
    carry_act = noise(splits[0], (SECTIONS, TOKENS, D), 1.0, 6.0, ((0, 16), (1, 16)))
    carry_act_tan = noise(splits[1], (SECTIONS, TOKENS, D), 1.0, 6.0, ((0, 16), (1, 16)))
    carry_adj = noise(splits[2], (SECTIONS, TOKENS, D), 0.125, 0.75, ((0, 16), (1, 16)))
    carry_adj_tan = noise(splits[3], (SECTIONS, TOKENS, D), 0.125, 0.75, ((0, 16), (1, 16)))
    fresh_act = noise(splits[4], (TICKS, TOKENS, D), 1.0, 6.0, ((1, 16),))
    loss_cot = noise(splits[5], (TICKS, TOKENS, D), 0.125, 0.75, ((1, 16),))
    stash_act = noise(splits[6], (SECTIONS, TICKS, TOKENS, D), 1.0, 6.0, ((0, 16), (2, 16)))
    stash_act_tan = noise(splits[7], (SECTIONS, TICKS, TOKENS, D), 1.0, 6.0, ((0, 16), (2, 16)))
    norm_gain = jnp.clip(1.0 + 0.15 * jax.random.normal(splits[8], (SECTIONS, D), jnp.float32), 0.25, 1.75).astype(jnp.bfloat16)
    up_weight = noise(splits[9], (SECTIONS, D, FF), D ** -0.5, 0.125, ((0, 16), (2, 16)))
    down_weight = noise(splits[10], (SECTIONS, FF, D), FF ** -0.5, 0.09375, ((0, 16), (1, 16)))
    up_dir = noise(splits[11], (SECTIONS, D, FF), D ** -0.5, 0.125, ((0, 16), (2, 16)))
    down_dir = noise(splits[12], (SECTIONS, FF, D), FF ** -0.5, 0.09375, ((0, 16), (1, 16)))
    return dict(carry_act=carry_act, carry_act_tan=carry_act_tan, carry_adj=carry_adj, carry_adj_tan=carry_adj_tan, fresh_act=fresh_act, loss_cot=loss_cot, stash_act=stash_act, stash_act_tan=stash_act_tan, norm_gain=norm_gain, up_weight=up_weight, down_weight=down_weight, up_dir=up_dir, down_dir=down_dir)


sqrt_two_over_pi = 0.7978845608028654
cubic_coef = 0.044715
norm_eps = 1e-06

def gelu_parts(linear):
    inner_arg = sqrt_two_over_pi * (linear + cubic_coef * linear * linear * linear)
    first_slope = sqrt_two_over_pi * (1.0 + 3.0 * cubic_coef * linear * linear)
    second_slope = 6.0 * sqrt_two_over_pi * cubic_coef * linear
    tanh_value = jnp.tanh(inner_arg)
    sech_square = 1.0 - tanh_value * tanh_value
    gelu_value = 0.5 * linear * (1.0 + tanh_value)
    gelu_first = 0.5 * (1.0 + tanh_value) + 0.5 * linear * sech_square * first_slope
    gelu_second = sech_square * (first_slope - linear * tanh_value * first_slope * first_slope + 0.5 * linear * second_slope)
    return (gelu_value, gelu_first, gelu_second)

def matrix_product(left, right):
    return jnp.dot(left, right, preferred_element_type=jnp.float32)

def product_last(left, right):
    return lax.dot_general(left, right, (((1,), (1,)), ((), ())), preferred_element_type=jnp.float32)

def product_first(left, right):
    return lax.dot_general(left, right, (((0,), (0,)), ((), ())), preferred_element_type=jnp.float32)

def norm_stats(rows, rows_tan):
    values = rows.astype(jnp.float32)
    values_tan = rows_tan.astype(jnp.float32)
    inverse = lax.rsqrt(lax.optimization_barrier(jnp.mean(values * values, axis=-1, keepdims=True)) + norm_eps)
    inverse_tan = -(inverse * inverse * inverse) * lax.optimization_barrier(jnp.mean(values * values_tan, axis=-1, keepdims=True))
    return (values, values_tan, inverse, inverse_tan)

def norm_rows(rows, rows_tan, gain_row):
    values, values_tan, inverse, inverse_tan = norm_stats(rows, rows_tan)
    gain_wide = gain_row.astype(jnp.float32)
    normed = (values * inverse * gain_wide).astype(jnp.bfloat16)
    normed_tan = ((values_tan * inverse + values * inverse_tan) * gain_wide).astype(jnp.bfloat16)
    return (normed, normed_tan)

def norm_back(rows, rows_tan, gain_row, arriving, arriving_tan, summed, summed_tan):
    values, values_tan, inverse, inverse_tan = norm_stats(rows, rows_tan)
    gain_wide = gain_row.astype(jnp.float32)
    weighted = summed * gain_wide
    weighted_tan = summed_tan * gain_wide
    moment = lax.optimization_barrier(jnp.mean(values * weighted, axis=-1, keepdims=True))
    moment_tan = lax.optimization_barrier(jnp.mean(values_tan * weighted + values * weighted_tan, axis=-1, keepdims=True))
    inverse_cube = inverse * inverse * inverse
    returned = arriving.astype(jnp.float32) + inverse * weighted - inverse_cube * values * moment
    returned_tan = arriving_tan.astype(jnp.float32) + inverse_tan * weighted + inverse * weighted_tan - 3.0 * inverse * inverse * inverse_tan * values * moment - inverse_cube * values_tan * moment - inverse_cube * values * moment_tan
    return (returned.astype(jnp.bfloat16), returned_tan.astype(jnp.bfloat16))

def branch_forward(normed, normed_tan, up_local, down_local, up_direction, down_direction):
    linear = matrix_product(normed, up_local)
    linear_tan = matrix_product(normed_tan, up_local) + matrix_product(normed, up_direction)
    gelu_value, gelu_first, gelu_second = gelu_parts(linear)
    hidden = gelu_value.astype(jnp.bfloat16)
    hidden_tan = (gelu_first * linear_tan).astype(jnp.bfloat16)
    partial_value = matrix_product(hidden, down_local)
    partial_tan = matrix_product(hidden_tan, down_local) + matrix_product(hidden, down_direction)
    return (partial_value, partial_tan)

def branch_backward(stash_normed, stash_normed_tan, adjoint_all, adjoint_all_tan, up_local, down_local, up_direction, down_direction):
    linear = matrix_product(stash_normed, up_local)
    linear_tan = matrix_product(stash_normed_tan, up_local) + matrix_product(stash_normed, up_direction)
    gelu_value, gelu_first, gelu_second = gelu_parts(linear)
    hidden = gelu_value.astype(jnp.bfloat16)
    hidden_tan = (gelu_first * linear_tan).astype(jnp.bfloat16)
    upstream = product_last(adjoint_all, down_local)
    upstream_tan = product_last(adjoint_all_tan, down_local) + product_last(adjoint_all, down_direction)
    deltas = (upstream * gelu_first).astype(jnp.bfloat16)
    deltas_tan = (upstream_tan * gelu_first + upstream * gelu_second * linear_tan).astype(jnp.bfloat16)
    curvature_down = product_first(hidden_tan, adjoint_all) + product_first(hidden, adjoint_all_tan)
    curvature_up = product_first(stash_normed_tan, deltas) + product_first(stash_normed, deltas_tan)
    partial_value = product_last(deltas, up_local)
    partial_tan = product_last(deltas_tan, up_local) + product_last(deltas, up_direction)
    return (partial_value, partial_tan, curvature_up, curvature_down)

def sum_slices(parts):
    rounded = lax.optimization_barrier(parts.astype(jnp.bfloat16)).astype(jnp.float32)
    return lax.optimization_barrier(jnp.sum(rounded, axis=0))

def one_section(packed):
    input_rows, input_tan, arriving, arriving_tan, stash_rows, stash_tan, gain_row, up_section, down_section, up_section_dir, down_section_dir = packed
    width = FF // N_DP
    up_sliced = jnp.moveaxis(up_section.reshape(D, N_DP, width), 1, 0)
    up_dir_sliced = jnp.moveaxis(up_section_dir.reshape(D, N_DP, width), 1, 0)
    down_sliced = down_section.reshape(N_DP, width, D)
    down_dir_sliced = down_section_dir.reshape(N_DP, width, D)
    normed, normed_tan = norm_rows(input_rows, input_tan, gain_row)

    def forward_slice(weights):
        return branch_forward(normed, normed_tan, weights[0], weights[1], weights[2], weights[3])
    partials = lax.map(forward_slice, (up_sliced, down_sliced, up_dir_sliced, down_dir_sliced))
    new_act = (input_rows.astype(jnp.float32) + sum_slices(partials[0])).astype(jnp.bfloat16)
    new_act_tan = (input_tan.astype(jnp.float32) + sum_slices(partials[1])).astype(jnp.bfloat16)
    stash_normed, stash_normed_tan = norm_rows(stash_rows, stash_tan, gain_row)

    def backward_slice(weights):
        return branch_backward(stash_normed, stash_normed_tan, arriving, arriving_tan, weights[0], weights[1], weights[2], weights[3])
    backs = lax.map(backward_slice, (up_sliced, down_sliced, up_dir_sliced, down_dir_sliced))
    summed = sum_slices(backs[0])
    summed_tan = sum_slices(backs[1])
    curvature_up = jnp.moveaxis(backs[2], 0, 1).reshape(D, FF)
    curvature_down = backs[3].reshape(FF, D)
    new_adj, new_adj_tan = norm_back(stash_rows, stash_tan, gain_row, arriving, arriving_tan, summed, summed_tan)
    return (new_act, new_act_tan, new_adj, new_adj_tan, curvature_up, curvature_down)

def reference(carry_act, carry_act_tan, carry_adj, carry_adj_tan, fresh_act, loss_cot, stash_act, stash_act_tan, norm_gain, up_weight, down_weight, up_dir, down_dir):
    activation, activation_tan = (carry_act, carry_act_tan)
    adjoint, adjoint_tan = (carry_adj, carry_adj_tan)
    total_up = jnp.zeros(up_weight.shape, jnp.float32)
    total_down = jnp.zeros(down_weight.shape, jnp.float32)
    for tick_index in range(TICKS):
        zero_rows = jnp.zeros_like(fresh_act[tick_index])
        input_rows = jnp.concatenate([fresh_act[tick_index][None], activation[:-1]], axis=0)
        input_tan = jnp.concatenate([zero_rows[None], activation_tan[:-1]], axis=0)
        arriving = jnp.concatenate([adjoint[1:], loss_cot[tick_index][None]], axis=0)
        arriving_tan = jnp.concatenate([adjoint_tan[1:], zero_rows[None]], axis=0)
        results = lax.map(one_section, (input_rows, input_tan, arriving, arriving_tan, stash_act[:, tick_index], stash_act_tan[:, tick_index], norm_gain, up_weight, down_weight, up_dir, down_dir))
        activation, activation_tan, adjoint, adjoint_tan = (results[0], results[1], results[2], results[3])
        total_up = total_up + results[4]
        total_down = total_down + results[5]
    return (activation, activation_tan, adjoint, adjoint_tan, total_up.astype(jnp.bfloat16), total_down.astype(jnp.bfloat16))
```

```python
import jax
import jax.numpy as jnp
from jax import lax
from jax.experimental import pallas as pl
from jax.experimental.pallas import tpu as pltpu
from jax.sharding import PartitionSpec as P

MESH = pl.DeviceIdType.MESH
F32, BF16 = jnp.float32, jnp.bfloat16

ROOT = 0.7978845608028654
CUBIC = 0.044715
EPS = 1e-06

D = 2304
W = 288
WP = 384
NC = 3
CW = D // NC
M1, A1, N1, M2, A2, N2 = range(6)
T1, P1, T2, P2 = range(4)


def gelu_parts(v):
    u = ROOT * (v + CUBIC * v * v * v)
    s1 = ROOT * (1.0 + 3.0 * CUBIC * v * v)
    s2 = 6.0 * ROOT * CUBIC * v
    th = jnp.tanh(u)
    sech = 1.0 - th * th
    g0 = 0.5 * v * (1.0 + th)
    g1 = 0.5 * (1.0 + th) + 0.5 * v * sech * s1
    g2 = sech * (s1 - v * th * s1 * s1 + 0.5 * v * s2)
    return g0, g1, g2


def stats(r, rt):
    inv = lax.rsqrt(jnp.mean(r * r, axis=-1, keepdims=True) + EPS)
    inv_t = -(inv * inv * inv) * jnp.mean(r * rt, axis=-1, keepdims=True)
    return inv, inv_t


def norm_pair(block, gain):
    r, rt = block[:8], block[8:]
    inv, inv_t = stats(r, rt)
    return jnp.concatenate([r * inv * gain, (rt * inv + r * inv_t) * gain], axis=0).astype(BF16)


def norm_back(block, arriving, grads, gain):
    x, xt = block[:8], block[8:]
    inv, inv_t = stats(x, xt)
    w, wt = grads[:8] * gain, grads[8:] * gain
    mu = jnp.mean(x * w, axis=-1, keepdims=True)
    mu_t = jnp.mean(xt * w + x * wt, axis=-1, keepdims=True)
    cube = inv * inv * inv
    out = arriving[:8] + inv * w - cube * x * mu
    out_t = (
        arriving[8:]
        + inv_t * w
        + inv * wt
        - 3.0 * inv * inv * inv_t * x * mu
        - cube * xt * mu
        - cube * x * mu_t
    )
    return out, out_t


def kernel(
    c_act, c_act_t, c_adj, c_adj_t, fresh, loss, stash, stash_t, gain_ref, up_h, down_h, upd_h, downd_h,
    o_act, o_act_t, o_adj, o_adj_t, o_up, o_down,
    G, ST, IN, CA, SH, WU, WV, AB, XT, XP, QC, ZC, OWN, PS, PR, YS, YR, ZS, ZR, FB, CU, CD, CO,
    w_sem, o_sem, lane_r, lane_s, part_r, part_s, pr_r, pr_s, yr_r, yr_s, zr_r, zr_s, in_r, in_s, ad_r, ad_s, st_r, st_s,
):
    s, d = lax.axis_index("section"), lax.axis_index("dp")
    z, y, c = lax.div(d, 8), lax.rem(lax.div(d, 2), 4), lax.rem(d, 2)
    zo, co = 1 - z, 1 - c
    s_up, s_dn = lax.rem(s + 1, 16), lax.rem(s + 15, 16)

    def dev(ss, zz, yy, cc):
        return (ss, zz * 8 + yy * 2 + cc)

    def slot(cc, yy, zz):
        return cc * 8 + yy * 2 + zz

    ynb = [y, lax.rem(y + 1, 4), lax.rem(y + 2, 4), lax.rem(y + 3, 4)]
    ysrc = [y, ynb[3], ynb[2], ynb[1]]
    partner = dev(s, z, y, co)
    across = dev(s, zo, y, c)
    own = [slot(c, y, z), slot(c, y, zo)]
    zhs = [z, zo]

    loads = []
    for i, (src, dst) in enumerate(((up_h, WU.at[pl.ds(0, W)]), (upd_h, WU.at[pl.ds(WP, W)]),
                                    (down_h, WV.at[pl.ds(0, W)]), (downd_h, WV.at[pl.ds(WP, W)]))):
        cp = pltpu.make_async_copy(src, dst, w_sem.at[i])
        cp.start()
        loads.append(cp)

    bar = pltpu.get_barrier_semaphore()
    peers = [partner, across] + [dev(s, z, ynb[i], c) for i in (1, 2, 3)]
    peers += [dev(ss, zz, y, c) for ss in (s_up, s_dn) for zz in (z, zo)]
    for peer in peers:
        pl.semaphore_signal(bar, inc=1, device_id=peer, device_id_type=MESH)

    sends = []

    def put(src, dst, ssem, rsem, to, keep=True):
        cp = pltpu.make_async_remote_copy(
            src_ref=src, dst_ref=dst, send_sem=ssem, recv_sem=rsem, device_id=to, device_id_type=MESH
        )
        cp.start()
        if keep:
            sends.append(cp)
        return cp

    def got(dst, ssem, rsem):
        pltpu.make_async_remote_copy(
            src_ref=dst, dst_ref=dst, send_sem=ssem, recv_sem=rsem, device_id=partner, device_id_type=MESH
        ).wait_recv()

    def sent(src, ssem, rsem):
        pltpu.make_async_remote_copy(
            src_ref=src, dst_ref=src, send_sem=ssem, recv_sem=rsem, device_id=partner, device_id_type=MESH
        ).wait_send()

    def pair(a, b):
        return jnp.concatenate([a.astype(F32), b.astype(F32)], axis=0).astype(BF16)

    gain = gain_ref[...].astype(F32)

    CA[0] = pair(c_act[0], c_act_t[0])
    CA[1] = pair(c_adj[0], c_adj_t[0])
    for k in range(2):
        ST[k, z] = pair(stash[0, k], stash_t[0, k])

    pl.semaphore_wait(bar, 9)

    @pl.when(s != 0)
    def _():
        for i in range(2):
            put(CA.at[1], G.at[A1, own[0]], ad_s.at[0, i], ad_r.at[0, z], dev(s_dn, zhs[i], y, c), keep=False)

    put(ST.at[0, z], ST.at[0, z], st_s.at[0], st_r.at[0], across)

    @pl.when(s != 15)
    def _():
        for i in range(2):
            put(CA.at[0], IN.at[0, z], in_s.at[0, i], in_r.at[0, z], dev(s_up, zhs[i], y, c), keep=False)

    zero = jnp.zeros((8, D), F32)

    @pl.when(s == 0)
    def _():
        for k in range(2):
            IN[k, z] = pair(fresh[k], zero)
            put(IN.at[k, z], IN.at[k, z], in_s.at[k, 2], in_r.at[k, z], across, keep=False)

    @pl.when(s == 15)
    def _():
        for k, g in enumerate((A1, A2)):
            G[g, own[0]] = pair(loss[k], zero)
            put(G.at[g, own[0]], G.at[g, own[0]], ad_s.at[k, 2], ad_r.at[k, z], across, keep=False)

    put(ST.at[1, z], ST.at[1, z], st_s.at[1], st_r.at[1], across)

    def wait_in(k, i):
        def go():
            got(IN.at[k, zhs[i]], in_s.at[k, 0], in_r.at[k, zhs[i]])

        if i == 0:
            pl.when(s != 0)(go)
        else:
            go()

    def wait_ad(k, i):
        def go():
            got(G.at[(A1, A2)[k], own[i]], ad_s.at[k, 0], ad_r.at[k, zhs[i]])

        if i == 0:
            pl.when(s != 15)(go)
        else:
            go()

    def send_own(g, i):
        ref = G.at[g, own[i]]
        for dd in (1, 3, 2):
            put(ref, ref, lane_s.at[g, dd - 1, i], lane_r.at[g, dd - 1, zhs[i]], dev(s, z, ynb[dd], c))
        put(ref, ref, part_s.at[g, 0, i], part_r.at[g, 0, zhs[i]], partner)

    def forward(g, i):
        for dd in (1, 3, 2):
            ref = G.at[g, slot(c, ysrc[dd], zhs[i])]
            got(ref, lane_s.at[g, dd - 1, i], lane_r.at[g, dd - 1, zhs[i]])
            put(ref, ref, part_s.at[g, dd, i], part_r.at[g, dd, zhs[i]], partner)

    def finish(g):
        for i in range(2):
            for dd in range(4):
                got(G.at[g, slot(co, ysrc[dd], zhs[i])], part_s.at[g, dd, i], part_r.at[g, dd, zhs[i]])

    def norm_to(g, ref, i):
        G[g, own[i]] = norm_pair(ref[zhs[i]].astype(F32), gain)

    def wide(g, weights):
        x = G[g].reshape(256, D)
        for j in range(3):
            AB[:, j * 256 : (j + 1) * 256] = lax.dot_general(
                x, weights[j * 256 : (j + 1) * 256, :], (((1,), (1,)), ((), ())), preferred_element_type=F32
            )
        r = AB[...].reshape(16, 16, 2 * WP)
        return r[:, :8, :WP], r[:, 8:, :WP] + r[:, :8, WP:]

    def left(X, v, vt):
        top = jnp.concatenate([v, jnp.zeros_like(v)], axis=2)
        low = jnp.concatenate([vt, v], axis=2)
        X[...] = jnp.concatenate([top, low], axis=1).reshape(256, 2 * WP).astype(BF16)

    def turned(v, vt):
        return jnp.concatenate([vt, v], axis=1).reshape(256, WP).astype(BF16)

    def rs_a(k, X, weights):
        for j in range(NC):
            wj = weights[:, j * CW : (j + 1) * CW]
            there = jnp.dot(X[pl.ds(pl.multiple_of(128 * co, 128), 128), :], wj, preferred_element_type=F32)
            PS[k, j] = there.astype(BF16)
            put(PS.at[k, j], PR.at[k, j], pr_s.at[k, j], pr_r.at[k, j], partner)
            OWN[k % 2, j] = jnp.dot(
                X[pl.ds(pl.multiple_of(128 * c, 128), 128), :], wj, preferred_element_type=F32
            )

    def rs_b(k):
        for j in range(NC):
            got(PR.at[k, j], pr_s.at[k, j], pr_r.at[k, j])
            total = OWN[k % 2, j] + PR[k, j].astype(F32)
            OWN[k % 2, j] = total
            YS[k, j] = total.astype(BF16).reshape(4, 32, CW)
            for dd in (2, 1, 3):
                put(YS.at[k, j, ynb[dd]], YR.at[k, j, dd - 1], yr_s.at[k, j, dd - 1], yr_r.at[k, j, dd - 1],
                    dev(s, z, ynb[dd], c))

    def rs_c(k):
        for j in range(NC):
            total = OWN[k % 2, j, pl.ds(pl.multiple_of(32 * y, 32), 32), :]
            for dd in (1, 3, 2):
                got(YR.at[k, j, dd - 1], yr_s.at[k, j, dd - 1], yr_r.at[k, j, dd - 1])
                total = total + YR[k, j, dd - 1].astype(F32)
            ZS[k, j] = total.astype(BF16).reshape(2, 16, CW)
            if k < 2:
                put(ZS.at[k, j], ZR.at[k, j], zr_s.at[k, j], zr_r.at[k, j], across)
            else:
                put(ZS.at[k, j, zo], ZR.at[k, j, zo], zr_s.at[k, j], zr_r.at[k, j], across)

    def rs_d(k):
        for j in range(NC):
            cols = slice(j * CW, (j + 1) * CW)
            if k < 2:
                got(ZR.at[k, j], zr_s.at[k, j], zr_r.at[k, j])
                FB[k % 2, :, :, cols] = ZS[k, j].astype(F32) + ZR[k, j].astype(F32)
            else:
                got(ZR.at[k, j, z], zr_s.at[k, j], zr_r.at[k, j])
                FB[k % 2, 0, :, cols] = ZS[k, j, z].astype(F32) + ZR[k, j, z].astype(F32)

    def forward_branch(tick):
        g, k = (N1, N2)[tick], (P1, P2)[tick]
        finish(g)
        a, at = wide(g, WU)
        g0, g1, _ = gelu_parts(a)
        left(XP, g0, g1 * at)
        rs_a(k, XP, WV)

    def backward_first(tick):
        g = (M1, M2)[tick]
        finish(g)
        return wide(g, WU)

    def backward_second(tick, b, bt):
        g, k = (A1, A2)[tick], (T1, T2)[tick]
        finish(g)
        g0, g1, g2 = gelu_parts(b)
        e, et = wide(g, WV)
        zv, zt = e * g1, et * g1 + e * g2 * bt
        left(XT, zv, zt)
        rs_a(k, XT, WU)
        QC[...] = turned(g0, g1 * bt)
        ZC[...] = turned(zv, zt)

    def curvature(tick):
        for lhs, acc, g, o in ((QC, CD, (A1, A2)[tick], 1), (ZC, CU, (M1, M2)[tick], 0)):
            lt = lhs[...].T[:W]
            x = G[g].reshape(256, D)
            for j in range(NC):
                cols = slice(j * CW, (j + 1) * CW)
                part = jnp.dot(lt, x[:, cols], preferred_element_type=F32)
                if tick == 0:
                    acc[:, cols] = part
                else:
                    CO[o, :, cols] = (acc[:, cols] + part).astype(BF16)

    norm_to(M1, ST.at[0], 0)
    send_own(M1, 0)
    wait_ad(0, 0)
    send_own(A1, 0)
    got(ST.at[0, zo], st_s.at[0], st_r.at[0])
    norm_to(M1, ST.at[0], 1)
    send_own(M1, 1)
    wait_ad(0, 1)
    send_own(A1, 1)
    forward(M1, 0)
    wait_in(0, 0)
    norm_to(N1, IN.at[0], 0)
    send_own(N1, 0)
    forward(A1, 0)
    wait_in(0, 1)
    norm_to(N1, IN.at[0], 1)
    send_own(N1, 1)
    for r in range(2):
        WU[r * WP + W : (r + 1) * WP, :] = jnp.zeros((WP - W, D), BF16)
        WV[r * WP + W : (r + 1) * WP, :] = jnp.zeros((WP - W, D), BF16)
    norm_to(M2, ST.at[1], 0)
    for cp in loads:
        cp.wait()
    forward(M1, 1)
    b, bt = backward_first(0)
    forward(A1, 1)
    backward_second(0, b, bt)
    forward(N1, 0)
    rs_b(T1)
    forward(N1, 1)
    forward_branch(0)
    rs_b(P1)
    got(ST.at[1, zo], st_s.at[1], st_r.at[1])
    norm_to(M2, ST.at[1], 1)
    send_own(M2, 0)
    send_own(M2, 1)
    rs_c(T1)
    curvature(0)

    rs_d(T1)
    for i in range(2):
        out, out_t = norm_back(ST[0, zhs[i]].astype(F32), G[A1, own[i]].astype(F32), FB[0, zhs[i]], gain)
        SH[0, zhs[i]] = jnp.concatenate([out, out_t], axis=0).astype(BF16)

    @pl.when(s != 0)
    def _():
        for i in range(2):
            put(SH.at[0, zhs[i]], G.at[A2, own[i]], ad_s.at[1, i], ad_r.at[1, zhs[i]], dev(s_dn, z, y, c), keep=False)

    rs_c(P1)
    rs_d(P1)
    SH[1] = (IN[0].astype(F32) + FB[1]).astype(BF16)

    @pl.when(s != 15)
    def _():
        for i in range(2):
            put(SH.at[1, zhs[i]], IN.at[1, zhs[i]], in_s.at[1, i], in_r.at[1, zhs[i]], dev(s_up, z, y, c), keep=False)

    forward(M2, 0)
    forward(M2, 1)
    for i in range(2):
        wait_ad(1, i)
        send_own(A2, i)
    for i in range(2):
        wait_in(1, i)
        norm_to(N2, IN.at[1], i)
        send_own(N2, i)
    b, bt = backward_first(1)
    forward(A2, 0)
    forward(A2, 1)
    backward_second(1, b, bt)
    forward(N2, 0)
    rs_b(T2)
    forward(N2, 1)
    forward_branch(1)
    rs_b(P2)
    curvature(1)
    outs = []
    for i, ref in enumerate((o_up, o_down)):
        cp = pltpu.make_async_copy(CO.at[i], ref, o_sem.at[i])
        cp.start()
        outs.append(cp)
    rs_c(T2)
    rs_c(P2)
    rs_d(T2)
    out, out_t = norm_back(ST[1, z].astype(F32), G[A2, own[0]].astype(F32), FB[0, 0], gain)
    o_adj[0] = out.astype(BF16)
    o_adj_t[0] = out_t.astype(BF16)
    rs_d(P2)
    result = IN[1, z].astype(F32) + FB[1, 0]
    o_act[0] = result[:8].astype(BF16)
    o_act_t[0] = result[8:].astype(BF16)

    for cp in outs:
        cp.wait()
    for cp in sends:
        cp.wait_send()

    @pl.when(s != 0)
    def _():
        for i in range(2):
            sent(CA.at[1], ad_s.at[0, i], ad_r.at[0, z])
            sent(SH.at[0, zhs[i]], ad_s.at[1, i], ad_r.at[1, z])

    @pl.when(s != 15)
    def _():
        for i in range(2):
            sent(CA.at[0], in_s.at[0, i], in_r.at[0, z])
            sent(SH.at[1, zhs[i]], in_s.at[1, i], in_r.at[1, z])

    @pl.when(s == 0)
    def _():
        for k in range(2):
            sent(IN.at[k, z], in_s.at[k, 2], in_r.at[k, z])

    @pl.when(s == 15)
    def _():
        for k, g in enumerate((A1, A2)):
            sent(G.at[g, own[0]], ad_s.at[k, 2], ad_r.at[k, z])


def shards(
    carry_act, carry_act_tan, carry_adj, carry_adj_tan, fresh_act, loss_cot, stash_act, stash_act_tan,
    norm_gain, up_weight, down_weight, up_dir, down_dir,
):
    rows = jax.ShapeDtypeStruct((1, 8, D), BF16)
    flat = jax.ShapeDtypeStruct((W, D), BF16)
    vmem, hbm = pl.BlockSpec(memory_space=pltpu.VMEM), pl.BlockSpec(memory_space=pl.ANY)
    dma = pltpu.SemaphoreType.DMA
    outs = pl.pallas_call(
        kernel,
        name="relay",
        out_shape=(rows, rows, rows, rows, flat, flat),
        in_specs=[vmem] * 9 + [hbm] * 4,
        out_specs=(vmem, vmem, vmem, vmem, hbm, hbm),
        scratch_shapes=[
            pltpu.VMEM((6, 16, 16, D), BF16),
            pltpu.VMEM((2, 2, 16, D), BF16),
            pltpu.VMEM((2, 2, 16, D), BF16),
            pltpu.VMEM((2, 16, D), BF16),
            pltpu.VMEM((2, 2, 16, D), BF16),
            pltpu.VMEM((2 * WP, D), BF16),
            pltpu.VMEM((2 * WP, D), BF16),
            pltpu.VMEM((256, 2 * WP), F32),
            pltpu.VMEM((256, 2 * WP), BF16),
            pltpu.VMEM((256, 2 * WP), BF16),
            pltpu.VMEM((256, WP), BF16),
            pltpu.VMEM((256, WP), BF16),
            pltpu.VMEM((2, NC, 128, CW), F32),
            pltpu.VMEM((4, NC, 128, CW), BF16),
            pltpu.VMEM((4, NC, 128, CW), BF16),
            pltpu.VMEM((4, NC, 4, 32, CW), BF16),
            pltpu.VMEM((4, NC, 3, 32, CW), BF16),
            pltpu.VMEM((4, NC, 2, 16, CW), BF16),
            pltpu.VMEM((4, NC, 2, 16, CW), BF16),
            pltpu.VMEM((2, 2, 16, D), F32),
            pltpu.VMEM((W, D), F32),
            pltpu.VMEM((W, D), F32),
            pltpu.VMEM((2, W, D), BF16),
            dma((4,)),
            dma((2,)),
            dma((6, 3, 2)),
            dma((6, 3, 2)),
            dma((6, 4, 2)),
            dma((6, 4, 2)),
            dma((4, NC)),
            dma((4, NC)),
            dma((4, NC, 3)),
            dma((4, NC, 3)),
            dma((4, NC)),
            dma((4, NC)),
            dma((2, 2)),
            dma((2, 3)),
            dma((2, 2)),
            dma((2, 3)),
            dma((2,)),
            dma((2,)),
        ],
        compiler_params=pltpu.CompilerParams(
            collective_id=0, has_side_effects=True, vmem_limit_bytes=60 * 1024 * 1024
        ),
    )(
        carry_act, carry_act_tan, carry_adj, carry_adj_tan, fresh_act, loss_cot, stash_act, stash_act_tan, norm_gain,
        up_weight[0].T, down_weight[0], up_dir[0].T, down_dir[0],
    )
    return outs[0], outs[1], outs[2], outs[3], outs[4].T[None], outs[5][None]


def solution(mesh):
    rows = P("section", "dp", None)
    in_specs = (
        rows, rows, rows, rows,
        P(None, "dp", None), P(None, "dp", None),
        P("section", None, "dp", None), P("section", None, "dp", None),
        P("section", None),
        P("section", None, "dp"), rows, P("section", None, "dp"), rows,
    )
    out_specs = (rows, rows, rows, rows, P("section", None, "dp"), rows)
    return jax.shard_map(shards, mesh=mesh, in_specs=in_specs, out_specs=out_specs, check_vma=False)
```

```python
import jax
import jax.numpy as jnp
from jax import lax
from jax.experimental import pallas as pl
from jax.experimental.pallas import tpu as pltpu
from jax.sharding import PartitionSpec as P

MESH = pl.DeviceIdType.MESH
F32, BF16 = jnp.float32, jnp.bfloat16

ROOT = 0.7978845608028654
CUBIC = 0.044715
EPS = 1e-06

D = 2304
W = 288
WP = 384
NC = 3
CW = D // NC
M1, A1, N1, M2, A2, N2 = range(6)
RING = {M1: (1, 0), A1: (3, 0), N1: (1, 0), M2: (3, 0), A2: (0, 0), N2: (0, 0)}
T1, P1, T2, P2 = range(4)


def gelu_parts(v):
    u = ROOT * (v + CUBIC * v * v * v)
    s1 = ROOT * (1.0 + 3.0 * CUBIC * v * v)
    s2 = 6.0 * ROOT * CUBIC * v
    th = jnp.tanh(u)
    sech = 1.0 - th * th
    g0 = 0.5 * v * (1.0 + th)
    g1 = 0.5 * (1.0 + th) + 0.5 * v * sech * s1
    g2 = sech * (s1 - v * th * s1 * s1 + 0.5 * v * s2)
    return g0, g1, g2


def stats(r, rt):
    inv = lax.rsqrt(jnp.mean(r * r, axis=-1, keepdims=True) + EPS)
    inv_t = -(inv * inv * inv) * jnp.mean(r * rt, axis=-1, keepdims=True)
    return inv, inv_t


def norm_pair(block, gain):
    r, rt = block[:8], block[8:]
    inv, inv_t = stats(r, rt)
    return jnp.concatenate([r * inv * gain, (rt * inv + r * inv_t) * gain], axis=0).astype(BF16)


def norm_back(block, arriving, grads, gain):
    x, xt = block[:8], block[8:]
    inv, inv_t = stats(x, xt)
    w, wt = grads[:8] * gain, grads[8:] * gain
    mu = jnp.mean(x * w, axis=-1, keepdims=True)
    mu_t = jnp.mean(xt * w + x * wt, axis=-1, keepdims=True)
    cube = inv * inv * inv
    out = arriving[:8] + inv * w - cube * x * mu
    out_t = (
        arriving[8:]
        + inv_t * w
        + inv * wt
        - 3.0 * inv * inv * inv_t * x * mu
        - cube * xt * mu
        - cube * x * mu_t
    )
    return out, out_t


def kernel(*refs):
    up_h, down_h, upd_h, downd_h = refs[9:13]
    o_act, o_act_t, o_adj, o_adj_t, o_up, o_down = refs[13:19]
    small = c_act, c_act_t, c_adj, c_adj_t, fresh, loss, stash, stash_t, gain_ref = refs[19:28]
    G, ST, IN, CA, SH, WU, WV, WUT, WVT, AB, GL, XT, XP, QC, ZC, OWN, PS, PR, YS, YR, ZS, ZR, FB, CU, CD = refs[28:53]
    (i_sem, w_sem, lane_r, lane_s, part_r, part_s, pr_r, pr_s, yr_r, yr_s, zr_r, zr_s,
     in_r, in_s, ad_r, ad_s, st_r, st_s) = refs[53:]
    s, d = lax.axis_index("section"), lax.axis_index("dp")
    z, y, c = lax.div(d, 8), lax.rem(lax.div(d, 2), 4), lax.rem(d, 2)
    zo, co = 1 - z, 1 - c
    s_up, s_dn = lax.rem(s + 1, 16), lax.rem(s + 15, 16)

    def dev(ss, zz, yy, cc):
        return (ss, zz * 8 + yy * 2 + cc)

    def slot(cc, yy, zz):
        return cc * 8 + yy * 2 + zz

    ynb = [y, lax.rem(y + 1, 4), lax.rem(y + 2, 4), lax.rem(y + 3, 4)]
    ysrc = [y, ynb[3], ynb[2], ynb[1]]
    partner = dev(s, z, y, co)
    across = dev(s, zo, y, c)
    own = [slot(c, y, z), slot(c, y, zo)]
    zhs = [z, zo]

    firsts = [pltpu.make_async_copy(a, b, i_sem.at[i]) for i, (a, b) in enumerate(zip(refs[:9], small))]
    for i in (6, 7, 2, 3, 0, 1, 8, 4, 5):
        firsts[i].start()

    loads = []
    for i, (src, dst) in enumerate(((up_h, WU.at[pl.ds(0, W)]), (upd_h, WU.at[pl.ds(WP, W)]),
                                    (down_h, WV.at[pl.ds(0, W)]), (downd_h, WV.at[pl.ds(WP, W)]))):
        cp = pltpu.make_async_copy(src, dst, w_sem.at[i])
        cp.start()
        loads.append(cp)

    bar = pltpu.get_barrier_semaphore()
    peers = [partner, across] + [dev(s, z, ynb[i], c) for i in (1, 2, 3)]
    peers += [dev(ss, zz, y, c) for ss in (s_up, s_dn) for zz in (z, zo)]
    for peer in peers:
        pl.semaphore_signal(bar, inc=1, device_id=peer, device_id_type=MESH)

    sends = []

    def put(src, dst, ssem, rsem, to, keep=True):
        cp = pltpu.make_async_remote_copy(
            src_ref=src, dst_ref=dst, send_sem=ssem, recv_sem=rsem, device_id=to, device_id_type=MESH
        )
        cp.start()
        if keep:
            sends.append(cp)
        return cp

    def got(dst, ssem, rsem):
        pltpu.make_async_remote_copy(
            src_ref=dst, dst_ref=dst, send_sem=ssem, recv_sem=rsem, device_id=partner, device_id_type=MESH
        ).wait_recv()

    def sent(src, ssem, rsem):
        pltpu.make_async_remote_copy(
            src_ref=src, dst_ref=src, send_sem=ssem, recv_sem=rsem, device_id=partner, device_id_type=MESH
        ).wait_send()

    def pair(a, b):
        return jnp.concatenate([a.astype(F32), b.astype(F32)], axis=0).astype(BF16)

    for cp in firsts:
        cp.wait()
    gain = gain_ref[...].astype(F32)

    CA[0] = pair(c_act[0], c_act_t[0])
    CA[1] = pair(c_adj[0], c_adj_t[0])
    for k in range(2):
        ST[k, z] = pair(stash[0, k], stash_t[0, k])

    pl.semaphore_wait(bar, 9)

    for i in range(2):

        @pl.when(s != 0)
        def _():
            put(CA.at[1], G.at[A1, own[0]], ad_s.at[0, i], ad_r.at[0, z], dev(s_dn, zhs[i], y, c), keep=False)

        if i == 1:
            continue

        @pl.when(s != 15)
        def _():
            put(CA.at[0], IN.at[0, z], in_s.at[0, i], in_r.at[0, z], dev(s_up, zhs[i], y, c), keep=False)

        put(ST.at[0, z], ST.at[0, z], st_s.at[0], st_r.at[0], across)

    @pl.when(s != 15)
    def _():
        put(CA.at[0], IN.at[0, z], in_s.at[0, 1], in_r.at[0, z], dev(s_up, zo, y, c), keep=False)

    zero = jnp.zeros((8, D), F32)

    @pl.when(s == 0)
    def _():
        for k in range(2):
            IN[k, z] = pair(fresh[k], zero)
            put(IN.at[k, z], IN.at[k, z], in_s.at[k, 2], in_r.at[k, z], across, keep=False)

    @pl.when(s == 15)
    def _():
        for k, g in enumerate((A1, A2)):
            G[g, own[0]] = pair(loss[k], zero)
            put(G.at[g, own[0]], G.at[g, own[0]], ad_s.at[k, 2], ad_r.at[k, z], across, keep=False)

    put(ST.at[1, z], ST.at[1, z], st_s.at[1], st_r.at[1], across)

    def wait_in(k, i, zz):
        def go():
            got(IN.at[k, zz], in_s.at[k, 0], in_r.at[k, zz])

        if k == 0 and i == 1:
            go()
        else:
            pl.when((s != 0) | (z != zz))(go)

    def wait_ad(k, i, zz):
        def go():
            ref = G.at[(A1, A2)[k], slot(c, y, zz)]
            got(ref, ad_s.at[k, 0], ad_r.at[k, zz])

        if k == 0 and i == 1:
            go()
        else:
            pl.when((s != 15) | (z != zz))(go)

    def send_own(g, i, zz):
        ref = G.at[g, slot(c, y, zz)]
        for dd in (1, 3) if RING[g][i] else (2, 1, 3):
            put(ref, ref, lane_s.at[g, dd - 1, i], lane_r.at[g, dd - 1, i], dev(s, z, ynb[dd], c))
        put(ref, ref, part_s.at[g, 0, i], part_r.at[g, 0, i], partner)

    def pass_on(g, i, zz, dds):
        for dd in dds:
            ref = G.at[g, slot(c, ysrc[dd], zz)]
            got(ref, lane_s.at[g, dd - 1, i], lane_r.at[g, dd - 1, i])
            if RING[g][i] == dd:
                put(ref, ref, lane_s.at[g, 1, i], lane_r.at[g, 1, i], dev(s, z, ynb[dd], c))
            put(ref, ref, part_s.at[g, dd, i], part_r.at[g, dd, i], partner)

    def near(g, i, zz):
        pass_on(g, i, zz, (1, 3))

    def far(g, i, zz):
        pass_on(g, i, zz, (2,))

    def both(g, i, zz):
        pass_on(g, i, zz, (1, 3, 2))

    def finish(g, order):
        for i in range(2):
            for dd in range(4):
                got(G.at[g, slot(co, ysrc[dd], order[i])], part_s.at[g, dd, i], part_r.at[g, dd, i])

    def norm_to(g, ref, zz):
        G[g, slot(c, y, zz)] = norm_pair(ref[zz].astype(F32), gain)

    def turn(weights, turned_weights):
        for j in range(9):
            cols = slice(j * 256, (j + 1) * 256)
            turned_weights[cols, :] = weights[:, cols].T

    def wide(n, g, weights, cc):
        x = G[g, pl.ds(8 * cc, 8)].reshape(128, D)
        for j in range(3):
            cols = slice(j * 256, (j + 1) * 256)
            AB[n, pl.ds(pl.multiple_of(128 * cc, 128), 128), cols] = jnp.dot(
                x, weights[:, cols], preferred_element_type=F32
            )

    def widened(n):
        r = AB[n].reshape(16, 16, 2 * WP)
        return r[:, :8, :WP], r[:, 8:, :WP] + r[:, :8, WP:]

    def left(X, v, vt):
        top = jnp.concatenate([v, jnp.zeros_like(v)], axis=2)
        low = jnp.concatenate([vt, v], axis=2)
        X[...] = jnp.concatenate([top, low], axis=1).reshape(256, 2 * WP).astype(BF16)

    def turned(v, vt):
        return jnp.concatenate([vt, v], axis=1).reshape(256, WP).astype(BF16)

    def reduce_a(k, X, weights):
        for j in range(NC):
            wj = weights[:, j * CW : (j + 1) * CW]
            there = jnp.dot(X[pl.ds(pl.multiple_of(128 * co, 128), 128), :], wj, preferred_element_type=F32)
            PS[k, j] = there.astype(BF16)
            put(PS.at[k, j], PR.at[k, j], pr_s.at[k, j], pr_r.at[k, j], partner)

    def reduce_b(k, X, weights, zz):
        for j in range(NC):
            wj = weights[:, j * CW : (j + 1) * CW]
            here = jnp.dot(X[pl.ds(pl.multiple_of(128 * c, 128), 128), :], wj, preferred_element_type=F32)
            got(PR.at[k, j], pr_s.at[k, j], pr_r.at[k, j])
            total = here + PR[k, j].astype(F32)
            OWN[k % 2, j] = total
            YS[k, :, :, j] = total.astype(BF16).reshape(4, 2, 16, CW)
            reduce_y(k, 0, zz, j)

    def reduce_y(k, i, zz, j):
        for dd in (2, 1, 3):
            put(YS.at[k, ynb[dd], zz, j], YR.at[k, zz, dd - 1, j], yr_s.at[k, i, dd - 1, j], yr_r.at[k, i, dd - 1, j],
                dev(s, z, ynb[dd], c))

    def reduce_more(k, zz):
        for j in range(NC):
            reduce_y(k, 1, zz, j)

    def reduce_z(k, i, zz):
        for j in range(NC):
            for dd in (1, 3, 2):
                got(YR.at[k, zz, dd - 1, j], yr_s.at[k, i, dd - 1, j], yr_r.at[k, i, dd - 1, j])
            total = OWN[k % 2, j, pl.ds(pl.multiple_of(32 * y + 16 * zz, 16), 16), :]
            for dd in (1, 3, 2):
                total = total + YR[k, zz, dd - 1, j].astype(F32)
            if k < 2 or i == 0:
                ZS[k, zz, j] = total.astype(BF16)
                put(ZS.at[k, zz, j], ZR.at[k, zz, j], zr_s.at[k, i, j], zr_r.at[k, i, j], across)
            else:
                FB[k % 2, zz, :, j * CW : (j + 1) * CW] = total

    def reduce_end(k, i, zz):
        for j in range(NC):
            got(ZR.at[k, zz, j], zr_s.at[k, i, j], zr_r.at[k, i, j])
            cols = slice(j * CW, (j + 1) * CW)
            mine = ZS[k, zz, j].astype(F32) if k < 2 else FB[k % 2, zz, :, cols]
            FB[k % 2, zz, :, cols] = mine + ZR[k, zz, j].astype(F32)

    def forward_branch(tick):
        a, at = widened(0)
        g0, g1, _ = gelu_parts(a)
        left(XP, g0, g1 * at)
        reduce_a((P1, P2)[tick], XP, WV)

    def forward_rest(tick):
        reduce_b((P1, P2)[tick], XP, WV, (0, zo)[tick])

    def backward_first():
        b, bt = widened(1)
        g0, g1, g2 = gelu_parts(b)
        GL[0], GL[1] = g1, g2 * bt
        QC[...] = turned(g0, g1 * bt)

    def backward_second(tick):
        e, et = widened(2)
        zv, zt = e * GL[0], et * GL[0] + e * GL[1]
        left(XT, zv, zt)
        reduce_a((T1, T2)[tick], XT, WU)
        ZC[...] = turned(zv, zt)
        reduce_b((T1, T2)[tick], XT, WU, (0, zo)[tick])

    def curvature(tick, which):
        for lhs, acc, g, o in (((QC, CD, (A1, A2)[tick], 1), (ZC, CU, (M1, M2)[tick], 0))[which],):
            lt = lhs[...].T[:W]
            x = G[g].reshape(256, D)
            for j in range(NC):
                cols = slice(j * CW, (j + 1) * CW)
                part = jnp.dot(lt, x[:, cols], preferred_element_type=F32)
                if tick == 0:
                    acc[:, cols] = part
                else:
                    (o_up, o_down)[o][:, cols] = (acc[:, cols] + part).astype(BF16)

    def next_adjoint(zz):
        out, out_t = norm_back(ST[0, zz].astype(F32), G[A1, slot(c, y, zz)].astype(F32), FB[0, zz], gain)
        SH[0, zz] = jnp.concatenate([out, out_t], axis=0).astype(BF16)

        @pl.when(s != 0)
        def _():
            put(SH.at[0, zz], G.at[A2, slot(c, y, zz)], ad_s.at[1, zz], ad_r.at[1, zz], dev(s_dn, z, y, c), keep=False)

    def next_input(zz):
        SH[1, zz] = (IN[0, zz].astype(F32) + FB[1, zz]).astype(BF16)

        @pl.when(s != 15)
        def _():
            put(SH.at[1, zz], IN.at[1, zz], in_s.at[1, zz], in_r.at[1, zz], dev(s_up, z, y, c), keep=False)

    with jax.named_scope("p00_norm_to_M1_ST_at_0_z"):
        norm_to(M1, ST.at[0], z)
    with jax.named_scope("p01_send_own_M1_0_z"):
        send_own(M1, 0, z)
    with jax.named_scope("p02_norm_to_M2_ST_at_1_z"):
        norm_to(M2, ST.at[1], z)
    with jax.named_scope("p03_send_own_M2_0_z"):
        send_own(M2, 0, z)
    for r in range(2):
        WU[r * WP + W : (r + 1) * WP, :] = jnp.zeros((WP - W, D), BF16)
        WV[r * WP + W : (r + 1) * WP, :] = jnp.zeros((WP - W, D), BF16)
    with jax.named_scope("p04_wait_ad_0_0_z"):
        wait_ad(0, 0, z)
    with jax.named_scope("p05_send_own_A1_0_z"):
        send_own(A1, 0, z)
    with jax.named_scope("p06_near_M1_0_z"):
        near(M1, 0, z)
    for cp in loads:
        cp.wait()
    with jax.named_scope("p07_turn_WU_WUT"):
        turn(WU, WUT)
    with jax.named_scope("p08_got_ST_at_0_zo_st_s_at_0"):
        got(ST.at[0, zo], st_s.at[0], st_r.at[0])
    with jax.named_scope("p09_norm_to_M1_ST_at_0_zo"):
        norm_to(M1, ST.at[0], zo)
    with jax.named_scope("p10_send_own_M1_1_zo"):
        send_own(M1, 1, zo)
    with jax.named_scope("p11_near_A1_0_z"):
        near(A1, 0, z)
    with jax.named_scope("p12_near_M2_0_z"):
        near(M2, 0, z)
    with jax.named_scope("p13_turn_WV_WVT"):
        turn(WV, WVT)
    with jax.named_scope("p14_wait_in_0_0_z"):
        wait_in(0, 0, z)
    with jax.named_scope("p15_norm_to_N1_IN_at_0_z"):
        norm_to(N1, IN.at[0], z)
    with jax.named_scope("p16_wait_ad_0_1_zo"):
        wait_ad(0, 1, zo)
    with jax.named_scope("p17_send_own_A1_1_zo"):
        send_own(A1, 1, zo)
    with jax.named_scope("p18_send_own_N1_0_z"):
        send_own(N1, 0, z)
    with jax.named_scope("p19_far_M1_0_z"):
        far(M1, 0, z)
    with jax.named_scope("p20_both_M1_1_zo"):
        both(M1, 1, zo)
    with jax.named_scope("p21_wide_1_M1_WUT_c"):
        wide(1, M1, WUT, c)
    with jax.named_scope("p22_wait_in_0_1_zo"):
        wait_in(0, 1, zo)
    with jax.named_scope("p23_norm_to_N1_IN_at_0_zo"):
        norm_to(N1, IN.at[0], zo)
    with jax.named_scope("p24_send_own_N1_1_zo"):
        send_own(N1, 1, zo)
    with jax.named_scope("p25_finish_M1_z_zo"):
        finish(M1, (z, zo))
    with jax.named_scope("p26_wide_1_M1_WUT_co"):
        wide(1, M1, WUT, co)
    with jax.named_scope("p27_far_A1_0_z"):
        far(A1, 0, z)
    with jax.named_scope("p28_both_A1_1_zo"):
        both(A1, 1, zo)
    with jax.named_scope("p29_near_N1_0_z"):
        near(N1, 0, z)
    with jax.named_scope("p30_got_ST_at_1_zo_st_s_at_1"):
        got(ST.at[1, zo], st_s.at[1], st_r.at[1])
    with jax.named_scope("p31_norm_to_M2_ST_at_1_zo"):
        norm_to(M2, ST.at[1], zo)
    with jax.named_scope("p32_send_own_M2_1_zo"):
        send_own(M2, 1, zo)
    with jax.named_scope("p33_backward_first"):
        backward_first()
    with jax.named_scope("p34_wide_2_A1_WVT_c"):
        wide(2, A1, WVT, c)
    with jax.named_scope("p35_finish_A1_z_zo"):
        finish(A1, (z, zo))
    with jax.named_scope("p36_wide_2_A1_WVT_co"):
        wide(2, A1, WVT, co)
    with jax.named_scope("p37_backward_second_0"):
        backward_second(0)
    with jax.named_scope("p38_reduce_more_T1_1"):
        reduce_more(T1, 1)
    with jax.named_scope("p39_far_N1_0_z"):
        far(N1, 0, z)
    with jax.named_scope("p40_both_N1_1_zo"):
        both(N1, 1, zo)
    with jax.named_scope("p41_wide_0_N1_WUT_c"):
        wide(0, N1, WUT, c)
    with jax.named_scope("p42_finish_N1_z_zo"):
        finish(N1, (z, zo))
    with jax.named_scope("p43_wide_0_N1_WUT_co"):
        wide(0, N1, WUT, co)
    with jax.named_scope("p44_forward_branch_0"):
        forward_branch(0)
    with jax.named_scope("p45_reduce_z_T1_0_0"):
        reduce_z(T1, 0, 0)
    with jax.named_scope("p46_forward_rest_0"):
        forward_rest(0)
    with jax.named_scope("p47_reduce_more_P1_1"):
        reduce_more(P1, 1)
    with jax.named_scope("p48_far_M2_0_z"):
        far(M2, 0, z)
    with jax.named_scope("p49_both_M2_1_zo"):
        both(M2, 1, zo)
    with jax.named_scope("p50_reduce_z_T1_1_1"):
        reduce_z(T1, 1, 1)
    with jax.named_scope("p51_curvature_0_0"):
        curvature(0, 0)
    with jax.named_scope("p52_reduce_end_T1_0_0"):
        reduce_end(T1, 0, 0)
    with jax.named_scope("p53_next_adjoint_0"):
        next_adjoint(0)
    with jax.named_scope("p54_reduce_z_P1_0_0"):
        reduce_z(P1, 0, 0)
    with jax.named_scope("p55_curvature_0_1"):
        curvature(0, 1)
    with jax.named_scope("p56_reduce_end_T1_1_1"):
        reduce_end(T1, 1, 1)
    with jax.named_scope("p57_next_adjoint_1"):
        next_adjoint(1)
    with jax.named_scope("p58_reduce_z_P1_1_1"):
        reduce_z(P1, 1, 1)
    with jax.named_scope("p59_wait_ad_1_0_0"):
        wait_ad(1, 0, 0)
    with jax.named_scope("p60_send_own_A2_0_0"):
        send_own(A2, 0, 0)
    with jax.named_scope("p61_reduce_end_P1_0_0"):
        reduce_end(P1, 0, 0)
    with jax.named_scope("p62_next_input_0"):
        next_input(0)
    with jax.named_scope("p63_wait_ad_1_1_1"):
        wait_ad(1, 1, 1)
    with jax.named_scope("p64_send_own_A2_1_1"):
        send_own(A2, 1, 1)
    with jax.named_scope("p65_wide_1_M2_WUT_c"):
        wide(1, M2, WUT, c)
    with jax.named_scope("p66_finish_M2_z_zo"):
        finish(M2, (z, zo))
    with jax.named_scope("p67_wide_1_M2_WUT_co"):
        wide(1, M2, WUT, co)
    with jax.named_scope("p68_reduce_end_P1_1_1"):
        reduce_end(P1, 1, 1)
    with jax.named_scope("p69_next_input_1"):
        next_input(1)
    with jax.named_scope("p70_backward_first"):
        backward_first()
    with jax.named_scope("p71_both_A2_0_0"):
        both(A2, 0, 0)
    with jax.named_scope("p72_wait_in_1_0_0"):
        wait_in(1, 0, 0)
    with jax.named_scope("p73_norm_to_N2_IN_at_1_0"):
        norm_to(N2, IN.at[1], 0)
    with jax.named_scope("p74_send_own_N2_0_0"):
        send_own(N2, 0, 0)
    with jax.named_scope("p75_both_A2_1_1"):
        both(A2, 1, 1)
    with jax.named_scope("p76_wide_2_A2_WVT_c"):
        wide(2, A2, WVT, c)
    with jax.named_scope("p77_wait_in_1_1_1"):
        wait_in(1, 1, 1)
    with jax.named_scope("p78_norm_to_N2_IN_at_1_1"):
        norm_to(N2, IN.at[1], 1)
    with jax.named_scope("p79_send_own_N2_1_1"):
        send_own(N2, 1, 1)
    with jax.named_scope("p80_finish_A2_0_1"):
        finish(A2, (0, 1))
    with jax.named_scope("p81_wide_2_A2_WVT_co"):
        wide(2, A2, WVT, co)
    with jax.named_scope("p82_backward_second_1"):
        backward_second(1)
    with jax.named_scope("p83_reduce_more_T2_z"):
        reduce_more(T2, z)
    with jax.named_scope("p84_both_N2_0_0"):
        both(N2, 0, 0)
    with jax.named_scope("p85_both_N2_1_1"):
        both(N2, 1, 1)
    with jax.named_scope("p86_wide_0_N2_WUT_c"):
        wide(0, N2, WUT, c)
    with jax.named_scope("p87_finish_N2_0_1"):
        finish(N2, (0, 1))
    with jax.named_scope("p88_wide_0_N2_WUT_co"):
        wide(0, N2, WUT, co)
    with jax.named_scope("p89_forward_branch_1"):
        forward_branch(1)
    with jax.named_scope("p90_forward_rest_1"):
        forward_rest(1)
    with jax.named_scope("p91_reduce_more_P2_z"):
        reduce_more(P2, z)
    with jax.named_scope("p92_reduce_z_T2_0_zo"):
        reduce_z(T2, 0, zo)
    with jax.named_scope("p93_curvature_1_0"):
        curvature(1, 0)
    with jax.named_scope("p94_curvature_1_1"):
        curvature(1, 1)
    with jax.named_scope("p95_reduce_z_T2_1_z"):
        reduce_z(T2, 1, z)
    with jax.named_scope("p96_reduce_z_P2_0_zo"):
        reduce_z(P2, 0, zo)
    with jax.named_scope("p97_reduce_end_T2_0_z"):
        reduce_end(T2, 0, z)
    out, out_t = norm_back(ST[1, z].astype(F32), G[A2, own[0]].astype(F32), FB[0, z], gain)
    o_adj[0] = out.astype(BF16)
    o_adj_t[0] = out_t.astype(BF16)
    with jax.named_scope("p98_reduce_z_P2_1_z"):
        reduce_z(P2, 1, z)
    with jax.named_scope("p99_reduce_end_P2_0_z"):
        reduce_end(P2, 0, z)
    result = IN[1, z].astype(F32) + FB[1, z]
    o_act[0] = result[:8].astype(BF16)
    o_act_t[0] = result[8:].astype(BF16)

    for cp in sends:
        cp.wait_send()

    @pl.when(s != 0)
    def _():
        for i in range(2):
            sent(CA.at[1], ad_s.at[0, i], ad_r.at[0, z])
            sent(SH.at[0, i], ad_s.at[1, i], ad_r.at[1, z])

    @pl.when(s != 15)
    def _():
        for i in range(2):
            sent(CA.at[0], in_s.at[0, i], in_r.at[0, z])
            sent(SH.at[1, i], in_s.at[1, i], in_r.at[1, z])

    @pl.when(s == 0)
    def _():
        for k in range(2):
            sent(IN.at[k, z], in_s.at[k, 2], in_r.at[k, z])

    @pl.when(s == 15)
    def _():
        for k, g in enumerate((A1, A2)):
            sent(G.at[g, own[0]], ad_s.at[k, 2], ad_r.at[k, z])


def results(*refs):
    srcs, dsts, sem = refs[:6], refs[6:12], refs[12]
    copies = [pltpu.make_async_copy(a, b, sem.at[i]) for i, (a, b) in enumerate(zip(srcs, dsts))]
    for cp in copies:
        cp.start()
    for cp in copies:
        cp.wait()


def shards(
    carry_act, carry_act_tan, carry_adj, carry_adj_tan, fresh_act, loss_cot, stash_act, stash_act_tan,
    norm_gain, up_weight, down_weight, up_dir, down_dir,
):
    rows = jax.ShapeDtypeStruct((1, 8, D), BF16)
    flat = jax.ShapeDtypeStruct((W, D), BF16)
    vmem, hbm = pl.BlockSpec(memory_space=pltpu.VMEM), pl.BlockSpec(memory_space=pl.ANY)
    dma = pltpu.SemaphoreType.DMA
    small = (
        carry_act, carry_act_tan, carry_adj, carry_adj_tan, fresh_act, loss_cot, stash_act, stash_act_tan, norm_gain,
    )
    outs = pl.pallas_call(
        kernel,
        name="relay",
        out_shape=[pltpu.VMEM(a.shape, a.dtype) for a in (rows, rows, rows, rows, flat, flat)],
        in_specs=[pl.BlockSpec(memory_space=pltpu.HBM)] * 13,
        out_specs=[vmem] * 6,
        scratch_shapes=[pltpu.VMEM(a.shape, a.dtype) for a in small]
        + [
            pltpu.VMEM((6, 16, 16, D), BF16),
            pltpu.VMEM((2, 2, 16, D), BF16),
            pltpu.VMEM((2, 2, 16, D), BF16),
            pltpu.VMEM((2, 16, D), BF16),
            pltpu.VMEM((2, 2, 16, D), BF16),
            pltpu.VMEM((2 * WP, D), BF16),
            pltpu.VMEM((2 * WP, D), BF16),
            pltpu.VMEM((D, 2 * WP), BF16),
            pltpu.VMEM((D, 2 * WP), BF16),
            pltpu.VMEM((3, 256, 2 * WP), F32),
            pltpu.VMEM((2, 16, 8, WP), F32),
            pltpu.VMEM((256, 2 * WP), BF16),
            pltpu.VMEM((256, 2 * WP), BF16),
            pltpu.VMEM((256, WP), BF16),
            pltpu.VMEM((256, WP), BF16),
            pltpu.VMEM((2, NC, 128, CW), F32),
            pltpu.VMEM((4, NC, 128, CW), BF16),
            pltpu.VMEM((4, NC, 128, CW), BF16),
            pltpu.VMEM((4, 4, 2, NC, 16, CW), BF16),
            pltpu.VMEM((4, 2, 3, NC, 16, CW), BF16),
            pltpu.VMEM((4, 2, NC, 16, CW), BF16),
            pltpu.VMEM((4, 2, NC, 16, CW), BF16),
            pltpu.VMEM((2, 2, 16, D), F32),
            pltpu.VMEM((W, D), F32),
            pltpu.VMEM((W, D), F32),
            dma((9,)),
            dma((4,)),
            dma((6, 3, 2)),
            dma((6, 3, 2)),
            dma((6, 4, 2)),
            dma((6, 4, 2)),
            dma((4, NC)),
            dma((4, NC)),
            dma((4, 2, 3, NC)),
            dma((4, 2, 3, NC)),
            dma((4, 2, NC)),
            dma((4, 2, NC)),
            dma((2, 2)),
            dma((2, 3)),
            dma((2, 2)),
            dma((2, 3)),
            dma((2,)),
            dma((2,)),
        ],
        compiler_params=pltpu.CompilerParams(
            collective_id=0, has_side_effects=True, vmem_limit_bytes=54 * 1024 * 1024
        ),
    )(
        *small,
        up_weight[0].T, down_weight[0], up_dir[0].T, down_dir[0],
    )
    outs = pl.pallas_call(
        results,
        name="results",
        out_shape=(rows, rows, rows, rows, flat, flat),
        in_specs=[vmem] * 6,
        out_specs=[hbm] * 6,
        scratch_shapes=[dma((6,))],
    )(*[pltpu.with_memory_space_constraint(a, pltpu.VMEM) for a in outs])
    return outs[0], outs[1], outs[2], outs[3], outs[4].T[None], outs[5][None]


def solution(mesh):
    rows = P("section", "dp", None)
    in_specs = (
        rows, rows, rows, rows,
        P(None, "dp", None), P(None, "dp", None),
        P("section", None, "dp", None), P("section", None, "dp", None),
        P("section", None),
        P("section", None, "dp"), rows, P("section", None, "dp"), rows,
    )
    out_specs = (rows, rows, rows, rows, P("section", None, "dp"), rows)
    return jax.shard_map(shards, mesh=mesh, in_specs=in_specs, out_specs=out_specs, check_vma=False)
```

```python
import jax
import jax.numpy as jnp
from jax import lax
from jax.experimental import pallas as pl
from jax.experimental.pallas import tpu as pltpu
from jax.sharding import PartitionSpec as P

MESH = pl.DeviceIdType.MESH
F32, BF16 = jnp.float32, jnp.bfloat16

ROOT = 0.7978845608028654
CUBIC = 0.044715
EPS = 1e-06

D = 2304
W = 288
WP = 384
NC = 3
CW = D // NC
M1, A1, N1, M2, A2, N2 = range(6)
RING = {M1: (1, 0), A1: (3, 0), N1: (1, 3), M2: (1, 3), A2: (0, 0), N2: (0, 0)}
T1, P1, T2, P2 = range(4)


def gelu_parts(v):
    u = ROOT * (v + CUBIC * v * v * v)
    s1 = ROOT * (1.0 + 3.0 * CUBIC * v * v)
    s2 = 6.0 * ROOT * CUBIC * v
    th = jnp.tanh(u)
    sech = 1.0 - th * th
    g0 = 0.5 * v * (1.0 + th)
    g1 = 0.5 * (1.0 + th) + 0.5 * v * sech * s1
    g2 = sech * (s1 - v * th * s1 * s1 + 0.5 * v * s2)
    return g0, g1, g2


def stats(r, rt):
    inv = lax.rsqrt(jnp.mean(r * r, axis=-1, keepdims=True) + EPS)
    inv_t = -(inv * inv * inv) * jnp.mean(r * rt, axis=-1, keepdims=True)
    return inv, inv_t


def norm_pair(block, gain):
    r, rt = block[:8], block[8:]
    inv, inv_t = stats(r, rt)
    return jnp.concatenate([r * inv * gain, (rt * inv + r * inv_t) * gain], axis=0).astype(BF16)


def norm_back(block, arriving, grads, gain):
    x, xt = block[:8], block[8:]
    inv, inv_t = stats(x, xt)
    w, wt = grads[:8] * gain, grads[8:] * gain
    mu = jnp.mean(x * w, axis=-1, keepdims=True)
    mu_t = jnp.mean(xt * w + x * wt, axis=-1, keepdims=True)
    cube = inv * inv * inv
    out = arriving[:8] + inv * w - cube * x * mu
    out_t = (
        arriving[8:]
        + inv_t * w
        + inv * wt
        - 3.0 * inv * inv * inv_t * x * mu
        - cube * xt * mu
        - cube * x * mu_t
    )
    return out, out_t


def kernel(*refs):
    up_h, down_h, upd_h, downd_h = refs[9:13]
    o_act, o_act_t, o_adj, o_adj_t, o_up, o_down = refs[13:19]
    small = c_act, c_act_t, c_adj, c_adj_t, fresh, loss, stash, stash_t, gain_ref = refs[19:28]
    G, ST, IN, CA, SH, WU, WV, WUT, WVT, AB, GL, XT, XP, QC, ZC, OWN, PS, PR, YS, YR, ZS, ZR, FB, CU, CD = refs[28:53]
    (i_sem, w_sem, lane_r, lane_s, part_r, part_s, pr_r, pr_s, yr_r, yr_s, zr_r, zr_s,
     in_r, in_s, ad_r, ad_s, st_r, st_s) = refs[53:]
    s, d = lax.axis_index("section"), lax.axis_index("dp")
    z, y, c = lax.div(d, 8), lax.rem(lax.div(d, 2), 4), lax.rem(d, 2)
    zo, co = 1 - z, 1 - c
    s_up, s_dn = lax.rem(s + 1, 16), lax.rem(s + 15, 16)

    def dev(ss, zz, yy, cc):
        return (ss, zz * 8 + yy * 2 + cc)

    def slot(cc, yy, zz):
        return zz * 8 + cc * 4 + yy

    ynb = [y, lax.rem(y + 1, 4), lax.rem(y + 2, 4), lax.rem(y + 3, 4)]
    ysrc = [y, ynb[3], ynb[2], ynb[1]]
    partner = dev(s, z, y, co)
    across = dev(s, zo, y, c)
    own = [slot(c, y, z), slot(c, y, zo)]
    zhs = [z, zo]

    firsts = [pltpu.make_async_copy(a, b, i_sem.at[i]) for i, (a, b) in enumerate(zip(refs[:9], small))]
    for i in (6, 7, 2, 3, 0, 1, 8, 4, 5):
        firsts[i].start()

    loads = []
    for i, (src, dst) in enumerate(((up_h, WU.at[pl.ds(0, W)]), (upd_h, WU.at[pl.ds(WP, W)]),
                                    (down_h, WV.at[pl.ds(0, W)]), (downd_h, WV.at[pl.ds(WP, W)]))):
        cp = pltpu.make_async_copy(src, dst, w_sem.at[i])
        cp.start()
        loads.append(cp)

    bar = pltpu.get_barrier_semaphore()
    peers = [partner, across] + [dev(s, z, ynb[i], c) for i in (1, 2, 3)]
    peers += [dev(ss, z, y, c) for ss in (s_up, s_dn)]
    for peer in peers:
        pl.semaphore_signal(bar, inc=1, device_id=peer, device_id_type=MESH)

    def put(src, dst, ssem, rsem, to):
        cp = pltpu.make_async_remote_copy(
            src_ref=src, dst_ref=dst, send_sem=ssem, recv_sem=rsem, device_id=to, device_id_type=MESH
        )
        cp.start()

    def got(dst, ssem, rsem):
        pltpu.make_async_remote_copy(
            src_ref=dst, dst_ref=dst, send_sem=ssem, recv_sem=rsem, device_id=partner, device_id_type=MESH
        ).wait_recv()

    def sent(src, ssem, rsem):
        pltpu.make_async_remote_copy(
            src_ref=src, dst_ref=src, send_sem=ssem, recv_sem=rsem, device_id=partner, device_id_type=MESH
        ).wait_send()

    def pair(a, b):
        return jnp.concatenate([a.astype(F32), b.astype(F32)], axis=0).astype(BF16)

    for cp in firsts:
        cp.wait()
    gain = gain_ref[...].astype(F32)

    CA[0] = pair(c_act[0], c_act_t[0])
    CA[1] = pair(c_adj[0], c_adj_t[0])
    for k in range(2):
        ST[k, z] = pair(stash[0, k], stash_t[0, k])

    pl.semaphore_wait(bar, 7)

    @pl.when(s != 0)
    def _():
        put(CA.at[1], G.at[A1, own[0]], ad_s.at[0, 0], ad_r.at[0, z], dev(s_dn, z, y, c))

    @pl.when(s != 15)
    def _():
        put(CA.at[0], IN.at[0, z], in_s.at[0, 0], in_r.at[0, z], dev(s_up, z, y, c))

    put(ST.at[0, z], ST.at[0, z], st_s.at[0], st_r.at[0], across)

    zero = jnp.zeros((8, D), F32)

    @pl.when(s == 0)
    def _():
        for k in range(2):
            IN[k, z] = pair(fresh[k], zero)

    @pl.when(s == 15)
    def _():
        for k, g in enumerate((A1, A2)):
            G[g, own[0]] = pair(loss[k], zero)

    def relay():
        ref = G.at[A1, own[0]]
        put(ref, ref, ad_s.at[0, 1], ad_r.at[0, z], across)

    def relay_in():
        ref = IN.at[0, z]
        put(ref, ref, in_s.at[0, 1], in_r.at[0, z], across)

    def relay_rest():
        put(ST.at[1, z], ST.at[1, z], st_s.at[1], st_r.at[1], across)

        @pl.when(s == 0)
        def _():
            put(IN.at[1, z], IN.at[1, z], in_s.at[1, 2], in_r.at[1, z], across)

        @pl.when(s == 15)
        def _():
            ref = G.at[A2, own[0]]
            put(ref, ref, ad_s.at[1, 2], ad_r.at[1, z], across)

    def wait_in(k, i, zz):
        def go():
            got(IN.at[k, zz], in_s.at[k, 0], in_r.at[k, zz])

        if k == 0 and i == 1:
            go()
        else:
            pl.when((s != 0) | (z != zz))(go)

    def wait_ad(k, i, zz):
        def go():
            ref = G.at[(A1, A2)[k], slot(c, y, zz)]
            got(ref, ad_s.at[k, 0], ad_r.at[k, zz])

        if k == 0 and i == 1:
            go()
        else:
            pl.when((s != 15) | (z != zz))(go)

    def send_own(g, i, zz):
        ref = G.at[g, slot(c, y, zz)]
        for dd in (1, 3) if RING[g][i] else (2, 1, 3):
            put(ref, ref, lane_s.at[g], lane_r.at[g, dd - 1, i], dev(s, z, ynb[dd], c))
        put(ref, ref, part_s.at[g], part_r.at[g, i], partner)

    def pass_on(g, i, zz, dds):
        for dd in dds:
            ref = G.at[g, slot(c, ysrc[dd], zz)]
            got(ref, lane_s.at[g], lane_r.at[g, dd - 1, i])
            if RING[g][i] == dd:
                put(ref, ref, lane_s.at[g], lane_r.at[g, 1, i], dev(s, z, ynb[dd], c))
            put(ref, ref, part_s.at[g], part_r.at[g, i], partner)

    def near(g, i, zz):
        pass_on(g, i, zz, (1, 3))

    def far(g, i, zz):
        pass_on(g, i, zz, (2,))

    def both(g, i, zz):
        pass_on(g, i, zz, (1, 3, 2))

    def finish(g, i, zz):
        got(G.at[g, pl.ds(slot(co, 0, zz), 4)], part_s.at[g], part_r.at[g, i])

    def norm_to(g, ref, zz):
        G[g, slot(c, y, zz)] = norm_pair(ref[zz].astype(F32), gain)

    def turn(weights, turned_weights):
        for j in range(9):
            cols = slice(j * 256, (j + 1) * 256)
            turned_weights[cols, :] = weights[:, cols].T

    def wide(n, g, weights, zz):
        x = G[g, pl.ds(8 * zz, 8)].reshape(128, D)
        for j in range(3):
            cols = slice(j * 256, (j + 1) * 256)
            AB[n, pl.ds(pl.multiple_of(128 * zz, 128), 128), cols] = jnp.dot(
                x, weights[:, cols], preferred_element_type=F32
            )

    def widened(n):
        r = AB[n].reshape(16, 16, 2 * WP)
        return r[:, :8, :WP], r[:, 8:, :WP] + r[:, :8, WP:]

    def left(X, v, vt):
        top = jnp.concatenate([v, jnp.zeros_like(v)], axis=2)
        low = jnp.concatenate([vt, v], axis=2)
        X[...] = jnp.concatenate([top, low], axis=1).reshape(256, 2 * WP).astype(BF16)

    def turned(v, vt):
        return jnp.concatenate([vt, v], axis=1).reshape(256, WP).astype(BF16)

    def lane(X, cc):
        return jnp.concatenate([X[pl.ds(pl.multiple_of(128 * h + 64 * cc, 64), 64), :] for h in range(2)], axis=0)

    def reduce_a(k, X, weights):
        for j in range(NC):
            wj = weights[:, j * CW : (j + 1) * CW]
            there = jnp.dot(lane(X, co), wj, preferred_element_type=F32)
            PS[k, j] = there.astype(BF16)
            put(PS.at[k, j], PR.at[k, j], pr_s.at[k], pr_r.at[k, j], partner)

    def reduce_b(k, X, weights, zz):
        for j in range(NC):
            wj = weights[:, j * CW : (j + 1) * CW]
            here = jnp.dot(lane(X, c), wj, preferred_element_type=F32)
            got(PR.at[k, j], pr_s.at[k], pr_r.at[k, j])
            total = here + PR[k, j].astype(F32)
            OWN[k % 2, j] = total
            YS[k, :, :, j] = total.astype(BF16).reshape(2, 4, 16, CW)
            reduce_y(k, 0, zz, j)

    def reduce_y(k, i, zz, j):
        for dd in (2, 1, 3):
            put(YS.at[k, zz, ynb[dd], j], YR.at[k, zz, j, dd - 1], yr_s.at[k], yr_r.at[k, i, j], dev(s, z, ynb[dd], c))

    def reduce_more(k, zz):
        for j in range(NC):
            reduce_y(k, 1, zz, j)

    def reduce_z(k, i, zz, chunks=range(NC)):
        for j in chunks:
            got(YR.at[k, zz, j], yr_s.at[k], yr_r.at[k, i, j])
            total = OWN[k % 2, j, pl.ds(pl.multiple_of(64 * zz + 16 * y, 16), 16), :]
            for dd in (1, 3, 2):
                total = total + YR[k, zz, j, dd - 1].astype(F32)
            if k < 2 or i == 0:
                ZS[k, zz, j] = total.astype(BF16)
                put(ZS.at[k, zz, j], ZR.at[k, zz, j], zr_s.at[k], zr_r.at[k, i, j], across)
            else:
                FB[k % 2, zz, :, j * CW : (j + 1) * CW] = total

    def reduce_end(k, i, zz):
        for j in range(NC):
            got(ZR.at[k, zz, j], zr_s.at[k], zr_r.at[k, i, j])
            cols = slice(j * CW, (j + 1) * CW)
            mine = ZS[k, zz, j].astype(F32) if k < 2 else FB[k % 2, zz, :, cols]
            FB[k % 2, zz, :, cols] = mine + ZR[k, zz, j].astype(F32)

    def forward_branch(tick):
        a, at = widened(0)
        g0, g1, _ = gelu_parts(a)
        left(XP, g0, g1 * at)
        reduce_a((P1, P2)[tick], XP, WV)

    def forward_rest(tick):
        reduce_b((P1, P2)[tick], XP, WV, (0, zo)[tick])

    def backward_first():
        b, bt = widened(1)
        g0, g1, g2 = gelu_parts(b)
        GL[0], GL[1] = g1, g2 * bt
        QC[...] = turned(g0, g1 * bt)

    def backward_second(tick):
        e, et = widened(2)
        zv, zt = e * GL[0], et * GL[0] + e * GL[1]
        left(XT, zv, zt)
        reduce_a((T1, T2)[tick], XT, WU)
        ZC[...] = turned(zv, zt)
        reduce_b((T1, T2)[tick], XT, WU, (0, zo)[tick])

    def curvature(tick, which):
        for lhs, acc, g, o in (((QC, CD, (A1, A2)[tick], 1), (ZC, CU, (M1, M2)[tick], 0))[which],):
            lt = lhs[...].T[:W]
            x = G[g].reshape(256, D)
            for j in range(NC):
                cols = slice(j * CW, (j + 1) * CW)
                part = jnp.dot(lt, x[:, cols], preferred_element_type=F32)
                if tick == 0:
                    acc[:, cols] = part
                else:
                    (o_up, o_down)[o][:, cols] = (acc[:, cols] + part).astype(BF16)

    def next_adjoint(zz):
        out, out_t = norm_back(ST[0, zz].astype(F32), G[A1, slot(c, y, zz)].astype(F32), FB[0, zz], gain)
        SH[0, zz] = jnp.concatenate([out, out_t], axis=0).astype(BF16)

        @pl.when(s != 0)
        def _():
            put(SH.at[0, zz], G.at[A2, slot(c, y, zz)], ad_s.at[1, zz], ad_r.at[1, zz], dev(s_dn, z, y, c))

    def next_input(zz):
        SH[1, zz] = (IN[0, zz].astype(F32) + FB[1, zz]).astype(BF16)

        @pl.when(s != 15)
        def _():
            put(SH.at[1, zz], IN.at[1, zz], in_s.at[1, zz], in_r.at[1, zz], dev(s_up, z, y, c))

    def settle_edges():
        sent(CA.at[0], ad_s.at[0, 1], ad_r.at[0, z])
        sent(CA.at[0], in_s.at[0, 1], in_r.at[0, z])

        @pl.when(s != 0)
        def _():
            sent(CA.at[1], ad_s.at[0, 0], ad_r.at[0, z])
            for i in range(2):
                sent(SH.at[0, i], ad_s.at[1, i], ad_r.at[1, z])

        @pl.when(s != 15)
        def _():
            sent(CA.at[0], in_s.at[0, 0], in_r.at[0, z])
            for i in range(2):
                sent(SH.at[1, i], in_s.at[1, i], in_r.at[1, z])

        @pl.when(s == 0)
        def _():
            sent(IN.at[1, z], in_s.at[1, 2], in_r.at[1, z])

        @pl.when(s == 15)
        def _():
            sent(G.at[A2, own[0]], ad_s.at[1, 2], ad_r.at[1, z])

    norm_to(M1, ST.at[0], z)
    send_own(M1, 0, z)
    norm_to(M2, ST.at[1], z)
    send_own(M2, 0, z)
    for r in range(2):
        WU[r * WP + W : (r + 1) * WP, :] = jnp.zeros((WP - W, D), BF16)
        WV[r * WP + W : (r + 1) * WP, :] = jnp.zeros((WP - W, D), BF16)
    wait_ad(0, 0, z)
    relay()
    send_own(A1, 0, z)
    wait_in(0, 0, z)
    relay_in()
    relay_rest()
    near(M1, 0, z)
    for cp in loads:
        cp.wait()
    turn(WU, WUT)
    got(ST.at[0, zo], st_s.at[0], st_r.at[0])
    norm_to(M1, ST.at[0], zo)
    send_own(M1, 1, zo)
    near(A1, 0, z)
    turn(WV, WVT)
    norm_to(N1, IN.at[0], z)
    wait_ad(0, 1, zo)
    send_own(A1, 1, zo)
    send_own(N1, 0, z)
    near(M2, 0, z)
    far(M1, 0, z)
    far(A1, 0, z)
    finish(M1, 0, z)
    wide(1, M1, WUT, z)
    both(M1, 1, zo)
    wait_in(0, 1, zo)
    norm_to(N1, IN.at[0], zo)
    send_own(N1, 1, zo)
    finish(A1, 0, z)
    wide(2, A1, WVT, z)
    finish(M1, 1, zo)
    wide(1, M1, WUT, zo)
    backward_first()
    both(A1, 1, zo)
    near(N1, 0, z)
    got(ST.at[1, zo], st_s.at[1], st_r.at[1])
    norm_to(M2, ST.at[1], zo)
    send_own(M2, 1, zo)
    finish(A1, 1, zo)
    wide(2, A1, WVT, zo)
    near(N1, 1, zo)
    backward_second(0)
    reduce_more(T1, 1)
    far(N1, 0, z)
    far(N1, 1, zo)
    near(M2, 1, zo)
    finish(N1, 0, z)
    wide(0, N1, WUT, z)
    reduce_z(T1, 0, 0, (0,))
    finish(N1, 1, zo)
    wide(0, N1, WUT, zo)
    reduce_z(T1, 0, 0, (1,))
    forward_branch(0)
    reduce_z(T1, 0, 0, (2,))
    forward_rest(0)
    reduce_more(P1, 1)
    reduce_z(T1, 1, 1)
    far(M2, 0, z)
    curvature(0, 0)
    reduce_end(T1, 0, 0)
    next_adjoint(0)
    reduce_z(P1, 0, 0)
    curvature(0, 1)
    reduce_end(T1, 1, 1)
    next_adjoint(1)
    wait_ad(1, 0, 0)
    send_own(A2, 0, 0)
    far(M2, 1, zo)
    reduce_z(P1, 1, 1)
    finish(M2, 0, z)
    wide(1, M2, WUT, z)
    wait_ad(1, 1, 1)
    send_own(A2, 1, 1)
    reduce_end(P1, 0, 0)
    next_input(0)
    finish(M2, 1, zo)
    wide(1, M2, WUT, zo)
    backward_first()
    both(A2, 0, 0)
    reduce_end(P1, 1, 1)
    next_input(1)
    finish(A2, 0, 0)
    wide(2, A2, WVT, 0)
    wait_in(1, 0, 0)
    norm_to(N2, IN.at[1], 0)
    send_own(N2, 0, 0)
    both(A2, 1, 1)
    wait_in(1, 1, 1)
    norm_to(N2, IN.at[1], 1)
    send_own(N2, 1, 1)
    finish(A2, 1, 1)
    wide(2, A2, WVT, 1)
    backward_second(1)
    reduce_more(T2, z)
    both(N2, 0, 0)
    finish(N2, 0, 0)
    wide(0, N2, WUT, 0)
    both(N2, 1, 1)
    finish(N2, 1, 1)
    wide(0, N2, WUT, 1)
    forward_branch(1)
    forward_rest(1)
    reduce_more(P2, z)
    reduce_z(T2, 0, zo)
    curvature(1, 0)
    curvature(1, 1)
    settle_edges()
    reduce_z(T2, 1, z)
    reduce_z(P2, 0, zo)
    reduce_end(T2, 0, z)
    out, out_t = norm_back(ST[1, z].astype(F32), G[A2, own[0]].astype(F32), FB[0, z], gain)
    o_adj[0] = out.astype(BF16)
    o_adj_t[0] = out_t.astype(BF16)
    reduce_z(P2, 1, z)
    reduce_end(P2, 0, z)
    result = IN[1, z].astype(F32) + FB[1, z]
    o_act[0] = result[:8].astype(BF16)
    o_act_t[0] = result[8:].astype(BF16)

    for g in range(6):
        sent(G.at[g, pl.ds(0, 6)], lane_s.at[g], part_r.at[g, 0])
        sent(G.at[g, pl.ds(0, 8)], part_s.at[g], part_r.at[g, 0])
    for k in range(4):
        sent(PS.at[k], pr_s.at[k], pr_r.at[k, 0])
        sent(YS.at[k, :, pl.ds(0, 3)], yr_s.at[k], pr_r.at[k, 0])
        sent(ZS.at[k] if k < 2 else ZS.at[k, 0], zr_s.at[k], pr_r.at[k, 0])
    for k in range(2):
        sent(ST.at[k, z], st_s.at[k], st_r.at[k])


def results(*refs):
    srcs, dsts, sem = refs[:6], refs[6:12], refs[12]
    copies = [pltpu.make_async_copy(a, b, sem.at[i]) for i, (a, b) in enumerate(zip(srcs, dsts))]
    for cp in copies:
        cp.start()
    for cp in copies:
        cp.wait()


def shards(
    carry_act, carry_act_tan, carry_adj, carry_adj_tan, fresh_act, loss_cot, stash_act, stash_act_tan,
    norm_gain, up_weight, down_weight, up_dir, down_dir,
):
    rows = jax.ShapeDtypeStruct((1, 8, D), BF16)
    flat = jax.ShapeDtypeStruct((W, D), BF16)
    vmem, hbm = pl.BlockSpec(memory_space=pltpu.VMEM), pl.BlockSpec(memory_space=pl.ANY)
    dma = pltpu.SemaphoreType.DMA
    small = (
        carry_act, carry_act_tan, carry_adj, carry_adj_tan, fresh_act, loss_cot, stash_act, stash_act_tan, norm_gain,
    )
    outs = pl.pallas_call(
        kernel,
        name="relay",
        out_shape=[pltpu.VMEM(a.shape, a.dtype) for a in (rows, rows, rows, rows, flat, flat)],
        in_specs=[pl.BlockSpec(memory_space=pltpu.HBM)] * 13,
        out_specs=[vmem] * 6,
        scratch_shapes=[pltpu.VMEM(a.shape, a.dtype) for a in small]
        + [
            pltpu.VMEM((6, 16, 16, D), BF16),
            pltpu.VMEM((2, 2, 16, D), BF16),
            pltpu.VMEM((2, 2, 16, D), BF16),
            pltpu.VMEM((2, 16, D), BF16),
            pltpu.VMEM((2, 2, 16, D), BF16),
            pltpu.VMEM((2 * WP, D), BF16),
            pltpu.VMEM((2 * WP, D), BF16),
            pltpu.VMEM((D, 2 * WP), BF16),
            pltpu.VMEM((D, 2 * WP), BF16),
            pltpu.VMEM((3, 256, 2 * WP), F32),
            pltpu.VMEM((2, 16, 8, WP), F32),
            pltpu.VMEM((256, 2 * WP), BF16),
            pltpu.VMEM((256, 2 * WP), BF16),
            pltpu.VMEM((256, WP), BF16),
            pltpu.VMEM((256, WP), BF16),
            pltpu.VMEM((2, NC, 128, CW), F32),
            pltpu.VMEM((4, NC, 128, CW), BF16),
            pltpu.VMEM((4, NC, 128, CW), BF16),
            pltpu.VMEM((4, 2, 4, NC, 16, CW), BF16),
            pltpu.VMEM((4, 2, NC, 3, 16, CW), BF16),
            pltpu.VMEM((4, 2, NC, 16, CW), BF16),
            pltpu.VMEM((4, 2, NC, 16, CW), BF16),
            pltpu.VMEM((2, 2, 16, D), F32),
            pltpu.VMEM((W, D), F32),
            pltpu.VMEM((W, D), F32),
            dma((9,)),
            dma((4,)),
            dma((6, 3, 2)),
            dma((6,)),
            dma((6, 2)),
            dma((6,)),
            dma((4, NC)),
            dma((4,)),
            dma((4, 2, NC)),
            dma((4,)),
            dma((4, 2, NC)),
            dma((4,)),
            dma((2, 2)),
            dma((2, 3)),
            dma((2, 2)),
            dma((2, 3)),
            dma((2,)),
            dma((2,)),
        ],
        compiler_params=pltpu.CompilerParams(
            collective_id=0, has_side_effects=True, vmem_limit_bytes=54 * 1024 * 1024
        ),
    )(
        *small,
        up_weight[0].T, down_weight[0], up_dir[0].T, down_dir[0],
    )
    outs = pl.pallas_call(
        results,
        name="results",
        out_shape=(rows, rows, rows, rows, flat, flat),
        in_specs=[vmem] * 6,
        out_specs=[hbm] * 6,
        scratch_shapes=[dma((6,))],
    )(*[pltpu.with_memory_space_constraint(a, pltpu.VMEM) for a in outs])
    return outs[0], outs[1], outs[2], outs[3], outs[4].T[None], outs[5][None]


def solution(mesh):
    rows = P("section", "dp", None)
    in_specs = (
        rows, rows, rows, rows,
        P(None, "dp", None), P(None, "dp", None),
        P("section", None, "dp", None), P("section", None, "dp", None),
        P("section", None),
        P("section", None, "dp"), rows, P("section", None, "dp"), rows,
    )
    out_specs = (rows, rows, rows, rows, P("section", None, "dp"), rows)
    return jax.shard_map(shards, mesh=mesh, in_specs=in_specs, out_specs=out_specs, check_vma=False)
```

```python
import jax
import jax.numpy as jnp
from jax import lax
from jax.experimental import pallas as pl
from jax.experimental.pallas import tpu as pltpu
from jax.sharding import PartitionSpec as P

MESH = pl.DeviceIdType.MESH
F32, BF16 = jnp.float32, jnp.bfloat16

ROOT = 0.7978845608028654
CUBIC = 0.044715
EPS = 1e-06

D = 2304
W = 288
WP = 384
NC = 3
CW = D // NC
M1, A1, N1, M2, A2, N2 = range(6)
RING = {M1: (1, 0), A1: (3, 0), N1: (1, 3), M2: (1, 0), A2: (0, 0), N2: (0, 0)}
T1, P1, T2, P2 = range(4)


def gelu_parts(v):
    u = ROOT * (v + CUBIC * v * v * v)
    s1 = ROOT * (1.0 + 3.0 * CUBIC * v * v)
    s2 = 6.0 * ROOT * CUBIC * v
    th = jnp.tanh(u)
    sech = 1.0 - th * th
    g0 = 0.5 * v * (1.0 + th)
    g1 = 0.5 * (1.0 + th) + 0.5 * v * sech * s1
    g2 = sech * (s1 - v * th * s1 * s1 + 0.5 * v * s2)
    return g0, g1, g2


def stats(r, rt):
    inv = lax.rsqrt(jnp.mean(r * r, axis=-1, keepdims=True) + EPS)
    inv_t = -(inv * inv * inv) * jnp.mean(r * rt, axis=-1, keepdims=True)
    return inv, inv_t


def norm_pair(block, gain):
    r, rt = block[:8], block[8:]
    inv, inv_t = stats(r, rt)
    return jnp.concatenate([r * inv * gain, (rt * inv + r * inv_t) * gain], axis=0).astype(BF16)


def norm_back(block, arriving, grads, gain):
    x, xt = block[:8], block[8:]
    inv, inv_t = stats(x, xt)
    w, wt = grads[:8] * gain, grads[8:] * gain
    mu = jnp.mean(x * w, axis=-1, keepdims=True)
    mu_t = jnp.mean(xt * w + x * wt, axis=-1, keepdims=True)
    cube = inv * inv * inv
    out = arriving[:8] + inv * w - cube * x * mu
    out_t = (
        arriving[8:]
        + inv_t * w
        + inv * wt
        - 3.0 * inv * inv * inv_t * x * mu
        - cube * xt * mu
        - cube * x * mu_t
    )
    return out, out_t


def kernel(*refs):
    up_h, down_h, upd_h, downd_h = refs[9:13]
    o_act, o_act_t, o_adj, o_adj_t, o_up, o_down = refs[13:19]
    small = c_act, c_act_t, c_adj, c_adj_t, fresh, loss, stash, stash_t, gain_ref = refs[19:28]
    G, ST, IN, CA, SH, WU, WV, WUT, WVT, AB, GL, XT, XP, QC, ZC, OWN, PS, PR, YS, YR, ZS, ZR, FB, CU, CD = refs[28:53]
    (i_sem, w_sem, lane_r, lane_s, part_r, part_s, pr_r, pr_s, yr_r, yr_s, zr_r, zr_s,
     in_r, in_s, ad_r, ad_s, st_r, st_s, next_r) = refs[53:]
    s, d = lax.axis_index("section"), lax.axis_index("dp")
    z, y, c = lax.div(d, 8), lax.rem(lax.div(d, 2), 4), lax.rem(d, 2)
    zo, co = 1 - z, 1 - c
    s_up, s_dn = lax.rem(s + 1, 16), lax.rem(s + 15, 16)

    def dev(ss, zz, yy, cc):
        return (ss, zz * 8 + yy * 2 + cc)

    def slot(cc, yy, zz):
        return zz * 8 + cc * 4 + yy

    ynb = [y, lax.rem(y + 1, 4), lax.rem(y + 2, 4), lax.rem(y + 3, 4)]
    ysrc = [y, ynb[3], ynb[2], ynb[1]]
    partner = dev(s, z, y, co)
    across = dev(s, zo, y, c)
    own = [slot(c, y, z), slot(c, y, zo)]
    zhs = [z, zo]

    firsts = [pltpu.make_async_copy(a, b, i_sem.at[i]) for i, (a, b) in enumerate(zip(refs[:9], small))]
    for i in (6, 7, 2, 3, 0, 1, 8, 4, 5):
        firsts[i].start()

    loads = []
    for i, (src, dst) in enumerate(((up_h, WU.at[pl.ds(0, W)]), (upd_h, WU.at[pl.ds(WP, W)]),
                                    (down_h, WV.at[pl.ds(0, W)]), (downd_h, WV.at[pl.ds(WP, W)]))):
        cp = pltpu.make_async_copy(src, dst, w_sem.at[i])
        cp.start()
        loads.append(cp)

    bar = pltpu.get_barrier_semaphore()
    peers = [partner, across] + [dev(s, z, ynb[i], c) for i in (1, 2, 3)]
    peers += [dev(ss, z, y, c) for ss in (s_up, s_dn)]
    for peer in peers:
        pl.semaphore_signal(bar, inc=1, device_id=peer, device_id_type=MESH)

    def put(src, dst, ssem, rsem, to):
        cp = pltpu.make_async_remote_copy(
            src_ref=src, dst_ref=dst, send_sem=ssem, recv_sem=rsem, device_id=to, device_id_type=MESH
        )
        cp.start()

    def got(dst, ssem, rsem):
        pltpu.make_async_remote_copy(
            src_ref=dst, dst_ref=dst, send_sem=ssem, recv_sem=rsem, device_id=partner, device_id_type=MESH
        ).wait_recv()

    def sent(src, ssem, rsem):
        pltpu.make_async_remote_copy(
            src_ref=src, dst_ref=src, send_sem=ssem, recv_sem=rsem, device_id=partner, device_id_type=MESH
        ).wait_send()

    def pair(a, b):
        return jnp.concatenate([a.astype(F32), b.astype(F32)], axis=0).astype(BF16)

    for cp in firsts:
        cp.wait()
    gain = gain_ref[...].astype(F32)

    CA[0] = pair(c_act[0], c_act_t[0])
    CA[1] = pair(c_adj[0], c_adj_t[0])
    for k in range(2):
        ST[k, z] = pair(stash[0, k], stash_t[0, k])

    pl.semaphore_wait(bar, 7)

    @pl.when(s != 0)
    def _():
        put(CA.at[1], G.at[A1, own[0]], ad_s.at[0, 0], ad_r.at[0, z], dev(s_dn, z, y, c))

    @pl.when(s != 15)
    def _():
        put(CA.at[0], IN.at[0, z], in_s.at[0, 0], in_r.at[0, z], dev(s_up, z, y, c))

    put(ST.at[0, z], ST.at[0, z], st_s.at[0], st_r.at[0], across)

    zero = jnp.zeros((8, D), F32)

    @pl.when(s == 0)
    def _():
        for k in range(2):
            IN[k, z] = pair(fresh[k], zero)

    @pl.when(s == 15)
    def _():
        for k, g in enumerate((A1, A2)):
            G[g, own[0]] = pair(loss[k], zero)

    def relay():
        ref = G.at[A1, own[0]]
        put(ref, ref, ad_s.at[0, 1], ad_r.at[0, z], across)

    def relay_in():
        ref = IN.at[0, z]
        put(ref, ref, in_s.at[0, 1], in_r.at[0, z], across)

    def relay_rest():
        put(ST.at[1, z], ST.at[1, z], st_s.at[1], st_r.at[1], across)

        @pl.when(s == 0)
        def _():
            for j in range(NC):
                ref = IN.at[1, z, :, j * CW : (j + 1) * CW]
                put(ref, ref, in_s.at[1, 2], next_r.at[z, j], across)

        @pl.when(s == 15)
        def _():
            ref = G.at[A2, own[0]]
            put(ref, ref, ad_s.at[1, 2], ad_r.at[1, z], across)

    def wait_in(k, i, zz):
        def go():
            if k == 0:
                got(IN.at[0, zz], in_s.at[0, 0], in_r.at[0, zz])
            else:
                for j in range(NC):
                    got(IN.at[1, zz, :, j * CW : (j + 1) * CW], in_s.at[1, 0], next_r.at[zz, j])

        if k == 0 and i == 1:
            go()
        else:
            pl.when((s != 0) | (z != zz))(go)

    def wait_ad(k, i, zz):
        def go():
            ref = G.at[(A1, A2)[k], slot(c, y, zz)]
            got(ref, ad_s.at[k, 0], ad_r.at[k, zz])

        if k == 0 and i == 1:
            go()
        else:
            pl.when((s != 15) | (z != zz))(go)

    def send_own(g, i, zz):
        ref = G.at[g, slot(c, y, zz)]
        for dd in (1, 3) if RING[g][i] else (2, 1, 3):
            put(ref, ref, lane_s.at[g], lane_r.at[g, dd - 1, i], dev(s, z, ynb[dd], c))
        put(ref, ref, part_s.at[g], part_r.at[g, i], partner)

    def pass_on(g, i, zz, dds):
        for dd in dds:
            ref = G.at[g, slot(c, ysrc[dd], zz)]
            got(ref, lane_s.at[g], lane_r.at[g, dd - 1, i])
            if RING[g][i] == dd:
                put(ref, ref, lane_s.at[g], lane_r.at[g, 1, i], dev(s, z, ynb[dd], c))
            put(ref, ref, part_s.at[g], part_r.at[g, i], partner)

    def near(g, i, zz):
        pass_on(g, i, zz, (1, 3))

    def far(g, i, zz):
        pass_on(g, i, zz, (2,))

    def both(g, i, zz):
        pass_on(g, i, zz, (1, 3, 2))

    def finish(g, i, zz):
        got(G.at[g, pl.ds(slot(co, 0, zz), 4)], part_s.at[g], part_r.at[g, i])

    def norm_to(g, ref, zz):
        G[g, slot(c, y, zz)] = norm_pair(ref[zz].astype(F32), gain)

    def turn(weights, turned_weights):
        for j in range(9):
            cols = slice(j * 256, (j + 1) * 256)
            turned_weights[cols, :] = weights[:, cols].T

    def wide(n, g, weights, zz):
        x = G[g, pl.ds(8 * zz, 8)].reshape(128, D)
        for j in range(3):
            cols = slice(j * 256, (j + 1) * 256)
            AB[n, pl.ds(pl.multiple_of(128 * zz, 128), 128), cols] = jnp.dot(
                x, weights[:, cols], preferred_element_type=F32
            )

    def widened(n):
        r = AB[n].reshape(16, 16, 2 * WP)
        return r[:, :8, :WP], r[:, 8:, :WP] + r[:, :8, WP:]

    def left(X, v, vt):
        top = jnp.concatenate([v, jnp.zeros_like(v)], axis=2)
        low = jnp.concatenate([vt, v], axis=2)
        X[...] = jnp.concatenate([top, low], axis=1).reshape(256, 2 * WP).astype(BF16)

    def turned(v, vt):
        return jnp.concatenate([vt, v], axis=1).reshape(256, WP).astype(BF16)

    def lane(X, cc):
        return jnp.concatenate([X[pl.ds(pl.multiple_of(128 * h + 64 * cc, 64), 64), :] for h in range(2)], axis=0)

    def reduce_a(k, X, weights):
        for j in range(NC):
            wj = weights[:, j * CW : (j + 1) * CW]
            there = jnp.dot(lane(X, co), wj, preferred_element_type=F32)
            PS[k, j] = there.astype(BF16)
            put(PS.at[k, j], PR.at[k, j], pr_s.at[k], pr_r.at[k, j], partner)

    def reduce_b(k, X, weights, zz):
        for j in range(NC):
            wj = weights[:, j * CW : (j + 1) * CW]
            here = jnp.dot(lane(X, c), wj, preferred_element_type=F32)
            got(PR.at[k, j], pr_s.at[k], pr_r.at[k, j])
            total = here + PR[k, j].astype(F32)
            OWN[k % 2, j] = total
            YS[k, :, :, j] = total.astype(BF16).reshape(2, 4, 16, CW)
            reduce_y(k, 0, zz, j)

    def reduce_y(k, i, zz, j):
        for dd in (2, 1, 3):
            put(YS.at[k, zz, ynb[dd], j], YR.at[k, zz, j, dd - 1], yr_s.at[k], yr_r.at[k, i, j], dev(s, z, ynb[dd], c))

    def reduce_more(k, zz):
        for j in range(NC):
            reduce_y(k, 1, zz, j)

    def reduce_z(k, i, zz, chunks=range(NC)):
        for j in chunks:
            got(YR.at[k, zz, j], yr_s.at[k], yr_r.at[k, i, j])
            total = OWN[k % 2, j, pl.ds(pl.multiple_of(64 * zz + 16 * y, 16), 16), :]
            for dd in (1, 3, 2):
                total = total + YR[k, zz, j, dd - 1].astype(F32)
            if k < 2 or i == 0:
                ZS[k, zz, j] = total.astype(BF16)
                put(ZS.at[k, zz, j], ZR.at[k, zz, j], zr_s.at[k], zr_r.at[k, i, j], across)
            else:
                FB[k % 2, zz, :, j * CW : (j + 1) * CW] = total

    def reduce_end(k, i, zz, chunks=range(NC)):
        for j in chunks:
            got(ZR.at[k, zz, j], zr_s.at[k], zr_r.at[k, i, j])
            cols = slice(j * CW, (j + 1) * CW)
            mine = ZS[k, zz, j].astype(F32) if k < 2 else FB[k % 2, zz, :, cols]
            FB[k % 2, zz, :, cols] = mine + ZR[k, zz, j].astype(F32)

    def forward_branch(tick):
        a, at = widened(0)
        g0, g1, _ = gelu_parts(a)
        left(XP, g0, g1 * at)
        reduce_a((P1, P2)[tick], XP, WV)

    def forward_rest(tick):
        reduce_b((P1, P2)[tick], XP, WV, (0, zo)[tick])

    def backward_first():
        b, bt = widened(1)
        g0, g1, g2 = gelu_parts(b)
        GL[0], GL[1] = g1, g2 * bt
        QC[...] = turned(g0, g1 * bt)

    def backward_second(tick):
        e, et = widened(2)
        zv, zt = e * GL[0], et * GL[0] + e * GL[1]
        left(XT, zv, zt)
        reduce_a((T1, T2)[tick], XT, WU)
        ZC[...] = turned(zv, zt)
        reduce_b((T1, T2)[tick], XT, WU, (0, zo)[tick])

    def curvature(tick, which):
        for lhs, acc, g, o in (((QC, CD, (A1, A2)[tick], 1), (ZC, CU, (M1, M2)[tick], 0))[which],):
            lt = lhs[...].T[:W]
            x = G[g].reshape(256, D)
            for j in range(NC):
                cols = slice(j * CW, (j + 1) * CW)
                part = jnp.dot(lt, x[:, cols], preferred_element_type=F32)
                if tick == 0:
                    acc[:, cols] = part
                else:
                    (o_up, o_down)[o][:, cols] = (acc[:, cols] + part).astype(BF16)

    def next_adjoint(zz):
        out, out_t = norm_back(ST[0, zz].astype(F32), G[A1, slot(c, y, zz)].astype(F32), FB[0, zz], gain)
        SH[0, zz] = jnp.concatenate([out, out_t], axis=0).astype(BF16)

        @pl.when(s != 0)
        def _():
            put(SH.at[0, zz], G.at[A2, slot(c, y, zz)], ad_s.at[1, zz], ad_r.at[1, zz], dev(s_dn, z, y, c))

    def next_input(zz):
        for j in range(NC):
            cols = slice(j * CW, (j + 1) * CW)
            reduce_end(P1, zz, zz, (j,))
            SH[1, zz, :, cols] = (IN[0, zz, :, cols].astype(F32) + FB[1, zz, :, cols]).astype(BF16)

            @pl.when(s != 15)
            def _():
                put(SH.at[1, zz, :, cols], IN.at[1, zz, :, cols], in_s.at[1, zz], next_r.at[zz, j], dev(s_up, z, y, c))

    def settle_edges():
        sent(CA.at[0], ad_s.at[0, 1], ad_r.at[0, z])
        sent(CA.at[0], in_s.at[0, 1], in_r.at[0, z])

        @pl.when(s != 0)
        def _():
            sent(CA.at[1], ad_s.at[0, 0], ad_r.at[0, z])
            for i in range(2):
                sent(SH.at[0, i], ad_s.at[1, i], ad_r.at[1, z])

        @pl.when(s != 15)
        def _():
            sent(CA.at[0], in_s.at[0, 0], in_r.at[0, z])
            for i in range(2):
                sent(SH.at[1, i], in_s.at[1, i], in_r.at[0, z])

        @pl.when(s == 0)
        def _():
            sent(IN.at[1, z], in_s.at[1, 2], in_r.at[0, z])

        @pl.when(s == 15)
        def _():
            sent(G.at[A2, own[0]], ad_s.at[1, 2], ad_r.at[1, z])

    norm_to(M1, ST.at[0], z)
    send_own(M1, 0, z)
    norm_to(M2, ST.at[1], z)
    send_own(M2, 0, z)
    for r in range(2):
        WU[r * WP + W : (r + 1) * WP, :] = jnp.zeros((WP - W, D), BF16)
        WV[r * WP + W : (r + 1) * WP, :] = jnp.zeros((WP - W, D), BF16)
    wait_ad(0, 0, z)
    relay()
    send_own(A1, 0, z)
    wait_in(0, 0, z)
    relay_in()
    relay_rest()
    near(M1, 0, z)
    for cp in loads:
        cp.wait()
    turn(WU, WUT)
    got(ST.at[0, zo], st_s.at[0], st_r.at[0])
    norm_to(M1, ST.at[0], zo)
    send_own(M1, 1, zo)
    near(A1, 0, z)
    turn(WV, WVT)
    norm_to(N1, IN.at[0], z)
    wait_ad(0, 1, zo)
    send_own(A1, 1, zo)
    send_own(N1, 0, z)
    far(M1, 0, z)
    far(A1, 0, z)
    finish(M1, 0, z)
    wide(1, M1, WUT, z)
    both(M1, 1, zo)
    wait_in(0, 1, zo)
    norm_to(N1, IN.at[0], zo)
    send_own(N1, 1, zo)
    finish(A1, 0, z)
    wide(2, A1, WVT, z)
    finish(M1, 1, zo)
    wide(1, M1, WUT, zo)
    backward_first()
    both(A1, 1, zo)
    near(N1, 0, z)
    finish(A1, 1, zo)
    wide(2, A1, WVT, zo)
    near(N1, 1, zo)
    backward_second(0)
    reduce_more(T1, 1)
    far(N1, 0, z)
    far(N1, 1, zo)
    got(ST.at[1, zo], st_s.at[1], st_r.at[1])
    norm_to(M2, ST.at[1], zo)
    finish(N1, 0, z)
    wide(0, N1, WUT, z)
    reduce_z(T1, 0, 0, (0,))
    finish(N1, 1, zo)
    wide(0, N1, WUT, zo)
    reduce_z(T1, 0, 0, (1,))
    forward_branch(0)
    reduce_z(T1, 0, 0, (2,))
    forward_rest(0)
    reduce_more(P1, 1)
    near(M2, 0, z)
    send_own(M2, 1, zo)
    reduce_z(T1, 1, 1)
    curvature(0, 0)
    reduce_end(T1, 0, 0)
    next_adjoint(0)
    reduce_z(P1, 0, 0)
    curvature(0, 1)
    reduce_end(T1, 1, 1)
    next_adjoint(1)
    reduce_z(P1, 1, 1)
    wait_ad(1, 0, 0)
    send_own(A2, 0, 0)
    far(M2, 0, z)
    finish(M2, 0, z)
    wide(1, M2, WUT, z)
    next_input(0)
    wait_ad(1, 1, 1)
    send_own(A2, 1, 1)
    both(M2, 1, zo)
    next_input(1)
    finish(M2, 1, zo)
    wide(1, M2, WUT, zo)
    both(A2, 0, 0)
    backward_first()
    wait_in(1, 0, 0)
    norm_to(N2, IN.at[1], 0)
    send_own(N2, 0, 0)
    finish(A2, 0, 0)
    wide(2, A2, WVT, 0)
    both(A2, 1, 1)
    wait_in(1, 1, 1)
    norm_to(N2, IN.at[1], 1)
    send_own(N2, 1, 1)
    finish(A2, 1, 1)
    wide(2, A2, WVT, 1)
    backward_second(1)
    reduce_more(T2, z)
    both(N2, 0, 0)
    both(N2, 1, 1)
    finish(N2, 0, 0)
    wide(0, N2, WUT, 0)
    finish(N2, 1, 1)
    wide(0, N2, WUT, 1)
    forward_branch(1)
    forward_rest(1)
    reduce_more(P2, z)
    reduce_z(T2, 0, zo)
    reduce_z(T2, 1, z)
    curvature(1, 0)
    curvature(1, 1)
    settle_edges()
    reduce_z(P2, 0, zo)
    reduce_end(T2, 0, z)
    out, out_t = norm_back(ST[1, z].astype(F32), G[A2, own[0]].astype(F32), FB[0, z], gain)
    o_adj[0] = out.astype(BF16)
    o_adj_t[0] = out_t.astype(BF16)
    reduce_z(P2, 1, z)
    reduce_end(P2, 0, z)
    result = IN[1, z].astype(F32) + FB[1, z]
    o_act[0] = result[:8].astype(BF16)
    o_act_t[0] = result[8:].astype(BF16)

    for g in range(6):
        sent(G.at[g, pl.ds(0, 6)], lane_s.at[g], part_r.at[g, 0])
        sent(G.at[g, pl.ds(0, 8)], part_s.at[g], part_r.at[g, 0])
    for k in range(4):
        sent(PS.at[k], pr_s.at[k], pr_r.at[k, 0])
        sent(YS.at[k, :, pl.ds(0, 3)], yr_s.at[k], pr_r.at[k, 0])
        sent(ZS.at[k] if k < 2 else ZS.at[k, 0], zr_s.at[k], pr_r.at[k, 0])
    for k in range(2):
        sent(ST.at[k, z], st_s.at[k], st_r.at[k])


def results(*refs):
    srcs, dsts, sem = refs[:6], refs[6:12], refs[12]
    copies = [pltpu.make_async_copy(a, b, sem.at[i]) for i, (a, b) in enumerate(zip(srcs, dsts))]
    for cp in copies:
        cp.start()
    for cp in copies:
        cp.wait()


def shards(
    carry_act, carry_act_tan, carry_adj, carry_adj_tan, fresh_act, loss_cot, stash_act, stash_act_tan,
    norm_gain, up_weight, down_weight, up_dir, down_dir,
):
    rows = jax.ShapeDtypeStruct((1, 8, D), BF16)
    flat = jax.ShapeDtypeStruct((W, D), BF16)
    vmem, hbm = pl.BlockSpec(memory_space=pltpu.VMEM), pl.BlockSpec(memory_space=pl.ANY)
    dma = pltpu.SemaphoreType.DMA
    small = (
        carry_act, carry_act_tan, carry_adj, carry_adj_tan, fresh_act, loss_cot, stash_act, stash_act_tan, norm_gain,
    )
    outs = pl.pallas_call(
        kernel,
        name="relay",
        out_shape=[pltpu.VMEM(a.shape, a.dtype) for a in (rows, rows, rows, rows, flat, flat)],
        in_specs=[pl.BlockSpec(memory_space=pltpu.HBM)] * 13,
        out_specs=[vmem] * 6,
        scratch_shapes=[pltpu.VMEM(a.shape, a.dtype) for a in small]
        + [
            pltpu.VMEM((6, 16, 16, D), BF16),
            pltpu.VMEM((2, 2, 16, D), BF16),
            pltpu.VMEM((2, 2, 16, D), BF16),
            pltpu.VMEM((2, 16, D), BF16),
            pltpu.VMEM((2, 2, 16, D), BF16),
            pltpu.VMEM((2 * WP, D), BF16),
            pltpu.VMEM((2 * WP, D), BF16),
            pltpu.VMEM((D, 2 * WP), BF16),
            pltpu.VMEM((D, 2 * WP), BF16),
            pltpu.VMEM((3, 256, 2 * WP), F32),
            pltpu.VMEM((2, 16, 8, WP), F32),
            pltpu.VMEM((256, 2 * WP), BF16),
            pltpu.VMEM((256, 2 * WP), BF16),
            pltpu.VMEM((256, WP), BF16),
            pltpu.VMEM((256, WP), BF16),
            pltpu.VMEM((2, NC, 128, CW), F32),
            pltpu.VMEM((4, NC, 128, CW), BF16),
            pltpu.VMEM((4, NC, 128, CW), BF16),
            pltpu.VMEM((4, 2, 4, NC, 16, CW), BF16),
            pltpu.VMEM((4, 2, NC, 3, 16, CW), BF16),
            pltpu.VMEM((4, 2, NC, 16, CW), BF16),
            pltpu.VMEM((4, 2, NC, 16, CW), BF16),
            pltpu.VMEM((2, 2, 16, D), F32),
            pltpu.VMEM((W, D), F32),
            pltpu.VMEM((W, D), F32),
            dma((9,)),
            dma((4,)),
            dma((6, 3, 2)),
            dma((6,)),
            dma((6, 2)),
            dma((6,)),
            dma((4, NC)),
            dma((4,)),
            dma((4, 2, NC)),
            dma((4,)),
            dma((4, 2, NC)),
            dma((4,)),
            dma((1, 2)),
            dma((2, 3)),
            dma((2, 2)),
            dma((2, 3)),
            dma((2,)),
            dma((2,)),
            dma((2, NC)),
        ],
        compiler_params=pltpu.CompilerParams(
            collective_id=0, has_side_effects=True, vmem_limit_bytes=54 * 1024 * 1024
        ),
    )(
        *small,
        up_weight[0].T, down_weight[0], up_dir[0].T, down_dir[0],
    )
    outs = pl.pallas_call(
        results,
        name="results",
        out_shape=(rows, rows, rows, rows, flat, flat),
        in_specs=[vmem] * 6,
        out_specs=[hbm] * 6,
        scratch_shapes=[dma((6,))],
    )(*[pltpu.with_memory_space_constraint(a, pltpu.VMEM) for a in outs])
    return outs[0], outs[1], outs[2], outs[3], outs[4].T[None], outs[5][None]


def solution(mesh):
    rows = P("section", "dp", None)
    in_specs = (
        rows, rows, rows, rows,
        P(None, "dp", None), P(None, "dp", None),
        P("section", None, "dp", None), P("section", None, "dp", None),
        P("section", None),
        P("section", None, "dp"), rows, P("section", None, "dp"), rows,
    )
    out_specs = (rows, rows, rows, rows, P("section", None, "dp"), rows)
    return jax.shard_map(shards, mesh=mesh, in_specs=in_specs, out_specs=out_specs, check_vma=False)
```

```python
import jax
import jax.numpy as jnp
from jax import lax
from jax.experimental import pallas as pl
from jax.experimental.pallas import tpu as pltpu
from jax.sharding import PartitionSpec as P

MESH = pl.DeviceIdType.MESH
F32, BF16 = jnp.float32, jnp.bfloat16

ROOT = 0.7978845608028654
CUBIC = 0.044715
EPS = 1e-06

D = 2304
W = 288
WP = 384
NC = 3
CW = D // NC
M1, A1, N1, M2, A2, N2 = range(6)
RING = {M1: (1, 0), A1: (3, 0), N1: (1, 3), M2: (1, 0), A2: (0, 0), N2: (0, 0)}
T1, P1, T2, P2 = range(4)


def gelu_parts(v):
    u = ROOT * (v + CUBIC * v * v * v)
    s1 = ROOT * (1.0 + 3.0 * CUBIC * v * v)
    s2 = 6.0 * ROOT * CUBIC * v
    th = jnp.tanh(u)
    sech = 1.0 - th * th
    g0 = 0.5 * v * (1.0 + th)
    g1 = 0.5 * (1.0 + th) + 0.5 * v * sech * s1
    g2 = sech * (s1 - v * th * s1 * s1 + 0.5 * v * s2)
    return g0, g1, g2


def stats(r, rt):
    inv = lax.rsqrt(jnp.mean(r * r, axis=-1, keepdims=True) + EPS)
    inv_t = -(inv * inv * inv) * jnp.mean(r * rt, axis=-1, keepdims=True)
    return inv, inv_t


def norm_pair(block, gain):
    r, rt = block[:8], block[8:]
    inv, inv_t = stats(r, rt)
    return jnp.concatenate([r * inv * gain, (rt * inv + r * inv_t) * gain], axis=0).astype(BF16)


def norm_back(block, arriving, grads, gain):
    x, xt = block[:8], block[8:]
    inv, inv_t = stats(x, xt)
    w, wt = grads[:8] * gain, grads[8:] * gain
    mu = jnp.mean(x * w, axis=-1, keepdims=True)
    mu_t = jnp.mean(xt * w + x * wt, axis=-1, keepdims=True)
    cube = inv * inv * inv
    out = arriving[:8] + inv * w - cube * x * mu
    out_t = (
        arriving[8:]
        + inv_t * w
        + inv * wt
        - 3.0 * inv * inv * inv_t * x * mu
        - cube * xt * mu
        - cube * x * mu_t
    )
    return out, out_t


def kernel(*refs):
    up_h, down_h, upd_h, downd_h = refs[9:13]
    o_act, o_act_t, o_adj, o_adj_t, o_up, o_down = refs[13:19]
    small = c_act, c_act_t, c_adj, c_adj_t, fresh, loss, stash, stash_t, gain_ref = refs[19:28]
    G, ST, IN, CA, SH, WU, WV, WUT, WVT, AB, GL, XT, XP, QC, ZC, OWN, PS, PR, YS, YR, ZS, ZR, FB, CU, CD = refs[28:53]
    (i_sem, w_sem, lane_r, lane_s, part_r, part_s, pr_r, pr_s, yr_r, yr_s, zr_r, zr_s,
     in_r, in_s, ad_r, ad_s, st_r, st_s, next_r) = refs[53:]
    s, d = lax.axis_index("section"), lax.axis_index("dp")
    z, y, c = lax.div(d, 8), lax.rem(lax.div(d, 2), 4), lax.rem(d, 2)
    zo, co = 1 - z, 1 - c
    s_up, s_dn = lax.rem(s + 1, 16), lax.rem(s + 15, 16)

    def dev(ss, zz, yy, cc):
        return (ss, zz * 8 + yy * 2 + cc)

    def slot(cc, yy, zz):
        return zz * 8 + cc * 4 + yy

    ynb = [y, lax.rem(y + 1, 4), lax.rem(y + 2, 4), lax.rem(y + 3, 4)]
    ysrc = [y, ynb[3], ynb[2], ynb[1]]
    partner = dev(s, z, y, co)
    across = dev(s, zo, y, c)
    own = [slot(c, y, z), slot(c, y, zo)]
    zhs = [z, zo]

    bar = pltpu.get_barrier_semaphore()
    peers = [partner, across] + [dev(s, z, ynb[i], c) for i in (1, 2, 3)]
    peers += [dev(ss, z, y, c) for ss in (s_up, s_dn)]
    for peer in peers:
        pl.semaphore_signal(bar, inc=1, device_id=peer, device_id_type=MESH)

    firsts = [pltpu.make_async_copy(a, b, i_sem.at[i]) for i, (a, b) in enumerate(zip(refs[:9], small))]
    for i in (6, 7, 2, 3, 0, 1, 8, 4, 5):
        firsts[i].start()

    loads = []
    for i, (src, dst) in enumerate(((up_h, WU.at[pl.ds(0, W)]), (upd_h, WU.at[pl.ds(WP, W)]),
                                    (down_h, WV.at[pl.ds(0, W)]), (downd_h, WV.at[pl.ds(WP, W)]))):
        cp = pltpu.make_async_copy(src, dst, w_sem.at[i])
        cp.start()
        loads.append(cp)

    def put(src, dst, ssem, rsem, to):
        cp = pltpu.make_async_remote_copy(
            src_ref=src, dst_ref=dst, send_sem=ssem, recv_sem=rsem, device_id=to, device_id_type=MESH
        )
        cp.start()

    def got(dst, ssem, rsem):
        pltpu.make_async_remote_copy(
            src_ref=dst, dst_ref=dst, send_sem=ssem, recv_sem=rsem, device_id=partner, device_id_type=MESH
        ).wait_recv()

    def sent(src, ssem, rsem):
        pltpu.make_async_remote_copy(
            src_ref=src, dst_ref=src, send_sem=ssem, recv_sem=rsem, device_id=partner, device_id_type=MESH
        ).wait_send()

    def pair(a, b):
        return jnp.concatenate([a.astype(F32), b.astype(F32)], axis=0).astype(BF16)

    for cp in firsts:
        cp.wait()
    gain = gain_ref[...].astype(F32)

    CA[0] = pair(c_act[0], c_act_t[0])
    CA[1] = pair(c_adj[0], c_adj_t[0])
    for k in range(2):
        ST[k, z] = pair(stash[0, k], stash_t[0, k])

    pl.semaphore_wait(bar, 7)

    @pl.when(s != 0)
    def _():
        put(CA.at[1], G.at[A1, own[0]], ad_s.at[0, 0], ad_r.at[0, z], dev(s_dn, z, y, c))

    @pl.when(s != 15)
    def _():
        put(CA.at[0], IN.at[0, z], in_s.at[0, 0], in_r.at[0, z], dev(s_up, z, y, c))

    put(ST.at[0, z], ST.at[0, z], st_s.at[0], st_r.at[0], across)

    zero = jnp.zeros((8, D), F32)

    @pl.when(s == 0)
    def _():
        for k in range(2):
            IN[k, z] = pair(fresh[k], zero)

    @pl.when(s == 15)
    def _():
        for k, g in enumerate((A1, A2)):
            G[g, own[0]] = pair(loss[k], zero)

    def relay():
        ref = G.at[A1, own[0]]
        put(ref, ref, ad_s.at[0, 1], ad_r.at[0, z], across)

    def relay_in():
        ref = IN.at[0, z]
        put(ref, ref, in_s.at[0, 1], in_r.at[0, z], across)

    def relay_rest():
        put(ST.at[1, z], ST.at[1, z], st_s.at[1], st_r.at[1], across)

        @pl.when(s == 0)
        def _():
            for j in range(NC):
                ref = IN.at[1, z, :, j * CW : (j + 1) * CW]
                put(ref, ref, in_s.at[1, 2], next_r.at[z, j], across)

        @pl.when(s == 15)
        def _():
            ref = G.at[A2, own[0]]
            put(ref, ref, ad_s.at[1, 2], ad_r.at[1, z], across)

    def wait_in(k, i, zz):
        def go():
            if k == 0:
                got(IN.at[0, zz], in_s.at[0, 0], in_r.at[0, zz])
            else:
                for j in range(NC):
                    got(IN.at[1, zz, :, j * CW : (j + 1) * CW], in_s.at[1, 0], next_r.at[zz, j])

        if k == 0 and i == 1:
            go()
        else:
            pl.when((s != 0) | (z != zz))(go)

    def wait_ad(k, i, zz):
        def go():
            ref = G.at[(A1, A2)[k], slot(c, y, zz)]
            got(ref, ad_s.at[k, 0], ad_r.at[k, zz])

        if k == 0 and i == 1:
            go()
        else:
            pl.when((s != 15) | (z != zz))(go)

    def send_own(g, i, zz):
        ref = G.at[g, slot(c, y, zz)]
        for dd in (1, 3) if RING[g][i] else (2, 1, 3):
            put(ref, ref, lane_s.at[0], lane_r.at[g, dd - 1, i], dev(s, z, ynb[dd], c))
        put(ref, ref, part_s.at[0], part_r.at[g, i], partner)

    def pass_on(g, i, zz, dds):
        for dd in dds:
            ref = G.at[g, slot(c, ysrc[dd], zz)]
            got(ref, lane_s.at[0], lane_r.at[g, dd - 1, i])
            if RING[g][i] == dd:
                put(ref, ref, lane_s.at[0], lane_r.at[g, 1, i], dev(s, z, ynb[dd], c))
            put(ref, ref, part_s.at[0], part_r.at[g, i], partner)

    def near(g, i, zz):
        pass_on(g, i, zz, (1, 3))

    def far(g, i, zz):
        pass_on(g, i, zz, (2,))

    def both(g, i, zz):
        pass_on(g, i, zz, (1, 3, 2))

    def finish(g, i, zz):
        got(G.at[g, pl.ds(slot(co, 0, zz), 4)], part_s.at[0], part_r.at[g, i])

    def norm_to(g, ref, zz):
        G[g, slot(c, y, zz)] = norm_pair(ref[zz].astype(F32), gain)

    def turn(weights, turned_weights):
        for j in range(9):
            cols = slice(j * 256, (j + 1) * 256)
            turned_weights[cols, :] = weights[:, cols].T

    def wide(n, g, weights, zz):
        x = G[g, pl.ds(8 * zz, 8)].reshape(128, D)
        for j in range(3):
            cols = slice(j * 256, (j + 1) * 256)
            AB[n, pl.ds(pl.multiple_of(128 * zz, 128), 128), cols] = jnp.dot(
                x, weights[:, cols], preferred_element_type=F32
            )

    def widened(n):
        r = AB[n].reshape(16, 16, 2 * WP)
        return r[:, :8, :WP], r[:, 8:, :WP] + r[:, :8, WP:]

    def left(X, v, vt):
        top = jnp.concatenate([v, jnp.zeros_like(v)], axis=2)
        low = jnp.concatenate([vt, v], axis=2)
        X[...] = jnp.concatenate([top, low], axis=1).reshape(256, 2 * WP).astype(BF16)

    def turned(v, vt):
        return jnp.concatenate([vt, v], axis=1).reshape(256, WP).astype(BF16)

    def lane(X, cc):
        return jnp.concatenate([X[pl.ds(pl.multiple_of(128 * h + 64 * cc, 64), 64), :] for h in range(2)], axis=0)

    def reduce_a(k, X, weights):
        for j in range(NC):
            wj = weights[:, j * CW : (j + 1) * CW]
            there = jnp.dot(lane(X, co), wj, preferred_element_type=F32)
            PS[k, j] = there.astype(BF16)
            put(PS.at[k, j], PR.at[k, j], pr_s.at[0], pr_r.at[k, j], partner)

    def reduce_b(k, X, weights, zz):
        for j in range(NC):
            wj = weights[:, j * CW : (j + 1) * CW]
            here = jnp.dot(lane(X, c), wj, preferred_element_type=F32)
            got(PR.at[k, j], pr_s.at[0], pr_r.at[k, j])
            total = here + PR[k, j].astype(F32)
            OWN[k % 2, j] = total
            YS[k, :, :, j] = total.astype(BF16).reshape(2, 4, 16, CW)
            reduce_y(k, 0, zz, j)

    def reduce_y(k, i, zz, j):
        for dd in (2, 1, 3):
            put(YS.at[k, zz, ynb[dd], j], YR.at[k, zz, j, dd - 1], yr_s.at[0], yr_r.at[k, i, j], dev(s, z, ynb[dd], c))

    def reduce_more(k, zz):
        for j in range(NC):
            reduce_y(k, 1, zz, j)

    def reduce_z(k, i, zz, chunks=range(NC)):
        for j in chunks:
            got(YR.at[k, zz, j], yr_s.at[0], yr_r.at[k, i, j])
            total = OWN[k % 2, j, pl.ds(pl.multiple_of(64 * zz + 16 * y, 16), 16), :]
            for dd in (1, 3, 2):
                total = total + YR[k, zz, j, dd - 1].astype(F32)
            if k < 2 or i == 0:
                ZS[k, zz, j] = total.astype(BF16)
                put(ZS.at[k, zz, j], ZR.at[k, zz, j], zr_s.at[0], zr_r.at[(k * 2 + i if k < 2 else k + 2) * NC + j], across)
            else:
                FB[k % 2, zz, :, j * CW : (j + 1) * CW] = total

    def reduce_end(k, i, zz, chunks=range(NC)):
        for j in chunks:
            got(ZR.at[k, zz, j], zr_s.at[0], zr_r.at[(k * 2 + i if k < 2 else k + 2) * NC + j])
            cols = slice(j * CW, (j + 1) * CW)
            mine = ZS[k, zz, j].astype(F32) if k < 2 else FB[k % 2, zz, :, cols]
            FB[k % 2, zz, :, cols] = mine + ZR[k, zz, j].astype(F32)

    def forward_branch(tick):
        a, at = widened(0)
        g0, g1, _ = gelu_parts(a)
        left(XP, g0, g1 * at)
        reduce_a((P1, P2)[tick], XP, WV)

    def forward_rest(tick):
        reduce_b((P1, P2)[tick], XP, WV, (0, zo)[tick])

    def backward_first():
        b, bt = widened(1)
        g0, g1, g2 = gelu_parts(b)
        GL[0], GL[1] = g1, g2 * bt
        QC[...] = turned(g0, g1 * bt)

    def backward_second(tick):
        e, et = widened(2)
        zv, zt = e * GL[0], et * GL[0] + e * GL[1]
        left(XT, zv, zt)
        reduce_a((T1, T2)[tick], XT, WU)
        ZC[...] = turned(zv, zt)
        reduce_b((T1, T2)[tick], XT, WU, (0, zo)[tick])

    def curvature(tick, which):
        for lhs, acc, g, o in (((QC, CD, (A1, A2)[tick], 1), (ZC, CU, (M1, M2)[tick], 0))[which],):
            lt = lhs[...].T[:W]
            x = G[g].reshape(256, D)
            for j in range(NC):
                cols = slice(j * CW, (j + 1) * CW)
                part = jnp.dot(lt, x[:, cols], preferred_element_type=F32)
                if tick == 0:
                    acc[:, cols] = part
                else:
                    (o_up, o_down)[o][:, cols] = (acc[:, cols] + part).astype(BF16)

    def next_adjoint(zz):
        out, out_t = norm_back(ST[0, zz].astype(F32), G[A1, slot(c, y, zz)].astype(F32), FB[0, zz], gain)
        SH[0, zz] = jnp.concatenate([out, out_t], axis=0).astype(BF16)

        @pl.when(s != 0)
        def _():
            put(SH.at[0, zz], G.at[A2, slot(c, y, zz)], ad_s.at[1, zz], ad_r.at[1, zz], dev(s_dn, z, y, c))

    def next_input(zz):
        for j in range(NC):
            cols = slice(j * CW, (j + 1) * CW)
            reduce_end(P1, zz, zz, (j,))
            SH[1, zz, :, cols] = (IN[0, zz, :, cols].astype(F32) + FB[1, zz, :, cols]).astype(BF16)

            @pl.when(s != 15)
            def _():
                put(SH.at[1, zz, :, cols], IN.at[1, zz, :, cols], in_s.at[1, zz], next_r.at[zz, j], dev(s_up, z, y, c))

    def settle_edges():
        sent(CA.at[0], ad_s.at[0, 1], ad_r.at[0, z])
        sent(CA.at[0], in_s.at[0, 1], in_r.at[0, z])

        @pl.when(s != 0)
        def _():
            sent(CA.at[1], ad_s.at[0, 0], ad_r.at[0, z])
            for i in range(2):
                sent(SH.at[0, i], ad_s.at[1, i], ad_r.at[1, z])

        @pl.when(s != 15)
        def _():
            sent(CA.at[0], in_s.at[0, 0], in_r.at[0, z])
            for i in range(2):
                sent(SH.at[1, i], in_s.at[1, i], in_r.at[0, z])

        @pl.when(s == 0)
        def _():
            sent(IN.at[1, z], in_s.at[1, 2], in_r.at[0, z])

        @pl.when(s == 15)
        def _():
            sent(G.at[A2, own[0]], ad_s.at[1, 2], ad_r.at[1, z])

    norm_to(M1, ST.at[0], z)
    send_own(M1, 0, z)
    norm_to(M2, ST.at[1], z)
    send_own(M2, 0, z)
    for r in range(2):
        WU[r * WP + W : (r + 1) * WP, :] = jnp.zeros((WP - W, D), BF16)
        WV[r * WP + W : (r + 1) * WP, :] = jnp.zeros((WP - W, D), BF16)
    wait_ad(0, 0, z)
    relay()
    send_own(A1, 0, z)
    wait_in(0, 0, z)
    relay_in()
    relay_rest()
    near(M1, 0, z)
    for cp in loads:
        cp.wait()
    turn(WU, WUT)
    got(ST.at[0, zo], st_s.at[0], st_r.at[0])
    norm_to(M1, ST.at[0], zo)
    send_own(M1, 1, zo)
    near(A1, 0, z)
    turn(WV, WVT)
    norm_to(N1, IN.at[0], z)
    wait_ad(0, 1, zo)
    send_own(A1, 1, zo)
    send_own(N1, 0, z)
    far(M1, 0, z)
    far(A1, 0, z)
    finish(M1, 0, z)
    wide(1, M1, WUT, z)
    both(M1, 1, zo)
    wait_in(0, 1, zo)
    norm_to(N1, IN.at[0], zo)
    send_own(N1, 1, zo)
    finish(A1, 0, z)
    wide(2, A1, WVT, z)
    finish(M1, 1, zo)
    wide(1, M1, WUT, zo)
    backward_first()
    both(A1, 1, zo)
    near(N1, 0, z)
    finish(A1, 1, zo)
    wide(2, A1, WVT, zo)
    near(N1, 1, zo)
    backward_second(0)
    reduce_more(T1, 1)
    far(N1, 0, z)
    far(N1, 1, zo)
    got(ST.at[1, zo], st_s.at[1], st_r.at[1])
    norm_to(M2, ST.at[1], zo)
    finish(N1, 0, z)
    wide(0, N1, WUT, z)
    reduce_z(T1, 0, 0, (0,))
    finish(N1, 1, zo)
    wide(0, N1, WUT, zo)
    reduce_z(T1, 0, 0, (1,))
    forward_branch(0)
    reduce_z(T1, 0, 0, (2,))
    forward_rest(0)
    reduce_more(P1, 1)
    near(M2, 0, z)
    send_own(M2, 1, zo)
    reduce_z(T1, 1, 1)
    curvature(0, 0)
    reduce_end(T1, 0, 0)
    next_adjoint(0)
    reduce_z(P1, 0, 0)
    curvature(0, 1)
    reduce_end(T1, 1, 1)
    next_adjoint(1)
    reduce_z(P1, 1, 1)
    wait_ad(1, 0, 0)
    send_own(A2, 0, 0)
    far(M2, 0, z)
    finish(M2, 0, z)
    wide(1, M2, WUT, z)
    next_input(0)
    wait_ad(1, 1, 1)
    send_own(A2, 1, 1)
    both(M2, 1, zo)
    next_input(1)
    finish(M2, 1, zo)
    wide(1, M2, WUT, zo)
    both(A2, 0, 0)
    backward_first()
    wait_in(1, 0, 0)
    norm_to(N2, IN.at[1], 0)
    send_own(N2, 0, 0)
    finish(A2, 0, 0)
    wide(2, A2, WVT, 0)
    both(A2, 1, 1)
    wait_in(1, 1, 1)
    norm_to(N2, IN.at[1], 1)
    send_own(N2, 1, 1)
    finish(A2, 1, 1)
    wide(2, A2, WVT, 1)
    backward_second(1)
    reduce_more(T2, z)
    both(N2, 0, 0)
    both(N2, 1, 1)
    finish(N2, 0, 0)
    wide(0, N2, WUT, 0)
    finish(N2, 1, 1)
    wide(0, N2, WUT, 1)
    forward_branch(1)
    forward_rest(1)
    reduce_more(P2, z)
    reduce_z(T2, 0, zo)
    reduce_z(T2, 1, z)
    curvature(1, 0)
    curvature(1, 1)
    settle_edges()
    reduce_z(P2, 0, zo)
    reduce_end(T2, 0, z)
    out, out_t = norm_back(ST[1, z].astype(F32), G[A2, own[0]].astype(F32), FB[0, z], gain)
    o_adj[0] = out.astype(BF16)
    o_adj_t[0] = out_t.astype(BF16)
    reduce_z(P2, 1, z)
    reduce_end(P2, 0, z)
    result = IN[1, z].astype(F32) + FB[1, z]
    o_act[0] = result[:8].astype(BF16)
    o_act_t[0] = result[8:].astype(BF16)

    sent(G.at[pl.ds(0, 3), pl.ds(0, 12)], lane_s.at[0], part_r.at[0, 0])
    sent(G.at[pl.ds(0, 3)], part_s.at[0], part_r.at[0, 0])
    sent(PS, pr_s.at[0], part_r.at[0, 0])
    sent(YS.at[:, :, pl.ds(0, 3)], yr_s.at[0], part_r.at[0, 0])
    sent(ZS.at[pl.ds(0, 3)], zr_s.at[0], part_r.at[0, 0])
    for k in range(2):
        sent(ST.at[k, z], st_s.at[k], st_r.at[k])


def results(*refs):
    srcs, dsts, sem = refs[:6], refs[6:12], refs[12]
    copies = [pltpu.make_async_copy(a, b, sem.at[i]) for i, (a, b) in enumerate(zip(srcs, dsts))]
    for cp in copies:
        cp.start()
    for cp in copies:
        cp.wait()


def shards(
    carry_act, carry_act_tan, carry_adj, carry_adj_tan, fresh_act, loss_cot, stash_act, stash_act_tan,
    norm_gain, up_weight, down_weight, up_dir, down_dir,
):
    rows = jax.ShapeDtypeStruct((1, 8, D), BF16)
    flat = jax.ShapeDtypeStruct((W, D), BF16)
    vmem, hbm = pl.BlockSpec(memory_space=pltpu.VMEM), pl.BlockSpec(memory_space=pl.ANY)
    dma = pltpu.SemaphoreType.DMA
    small = (
        carry_act, carry_act_tan, carry_adj, carry_adj_tan, fresh_act, loss_cot, stash_act, stash_act_tan, norm_gain,
    )
    outs = pl.pallas_call(
        kernel,
        name="relay",
        out_shape=[pltpu.VMEM(a.shape, a.dtype) for a in (rows, rows, rows, rows, flat, flat)],
        in_specs=[pl.BlockSpec(memory_space=pltpu.HBM)] * 13,
        out_specs=[vmem] * 6,
        scratch_shapes=[pltpu.VMEM(a.shape, a.dtype) for a in small]
        + [
            pltpu.VMEM((6, 16, 16, D), BF16),
            pltpu.VMEM((2, 2, 16, D), BF16),
            pltpu.VMEM((2, 2, 16, D), BF16),
            pltpu.VMEM((2, 16, D), BF16),
            pltpu.VMEM((2, 2, 16, D), BF16),
            pltpu.VMEM((2 * WP, D), BF16),
            pltpu.VMEM((2 * WP, D), BF16),
            pltpu.VMEM((D, 2 * WP), BF16),
            pltpu.VMEM((D, 2 * WP), BF16),
            pltpu.VMEM((3, 256, 2 * WP), F32),
            pltpu.VMEM((2, 16, 8, WP), F32),
            pltpu.VMEM((256, 2 * WP), BF16),
            pltpu.VMEM((256, 2 * WP), BF16),
            pltpu.VMEM((256, WP), BF16),
            pltpu.VMEM((256, WP), BF16),
            pltpu.VMEM((2, NC, 128, CW), F32),
            pltpu.VMEM((4, NC, 128, CW), BF16),
            pltpu.VMEM((4, NC, 128, CW), BF16),
            pltpu.VMEM((4, 2, 4, NC, 16, CW), BF16),
            pltpu.VMEM((4, 2, NC, 3, 16, CW), BF16),
            pltpu.VMEM((4, 2, NC, 16, CW), BF16),
            pltpu.VMEM((4, 2, NC, 16, CW), BF16),
            pltpu.VMEM((2, 2, 16, D), F32),
            pltpu.VMEM((W, D), F32),
            pltpu.VMEM((W, D), F32),
            dma((9,)),
            dma((4,)),
            dma((6, 3, 2)),
            dma((1,)),
            dma((6, 2)),
            dma((1,)),
            dma((4, NC)),
            dma((1,)),
            dma((4, 2, NC)),
            dma((1,)),
            dma((6 * NC,)),
            dma((1,)),
            dma((1, 2)),
            dma((2, 3)),
            dma((2, 2)),
            dma((2, 3)),
            dma((2,)),
            dma((2,)),
            dma((2, NC)),
        ],
        compiler_params=pltpu.CompilerParams(
            collective_id=0, has_side_effects=True, vmem_limit_bytes=54 * 1024 * 1024
        ),
    )(
        *small,
        up_weight[0].T, down_weight[0], up_dir[0].T, down_dir[0],
    )
    outs = pl.pallas_call(
        results,
        name="results",
        out_shape=(rows, rows, rows, rows, flat, flat),
        in_specs=[vmem] * 6,
        out_specs=[hbm] * 6,
        scratch_shapes=[dma((6,))],
    )(*[pltpu.with_memory_space_constraint(a, pltpu.VMEM) for a in outs])
    return outs[0], outs[1], outs[2], outs[3], outs[4].T[None], outs[5][None]


def solution(mesh):
    rows = P("section", "dp", None)
    in_specs = (
        rows, rows, rows, rows,
        P(None, "dp", None), P(None, "dp", None),
        P("section", None, "dp", None), P("section", None, "dp", None),
        P("section", None),
        P("section", None, "dp"), rows, P("section", None, "dp"), rows,
    )
    out_specs = (rows, rows, rows, rows, P("section", None, "dp"), rows)
    return jax.shard_map(shards, mesh=mesh, in_specs=in_specs, out_specs=out_specs, check_vma=False)
```
